8 devices in a mesh: ep: 8 (over z, y, x, core).
Axes of the slice: x: 2, y: 2, z: 1, core: 2. Of those that a mesh axis runs over, the one named last changes fastest.
Arguments:
- tokens: bfloat16 [4096, 512], P('ep')
- grad_out: bfloat16 [4096, 512], P('ep')
- expert_ids: int32 [4096, 2], P('ep')
- w_gate: bfloat16 [512, 8], replicated
- w_in: bfloat16 [8, 512, 2048], P('ep')
- w_out: bfloat16 [8, 2048, 512], P('ep')
Outputs:
- output 1: bfloat16 [4096, 512], P('ep')
- output 2: bfloat16 [4096, 512], P('ep')
- output 3: float32 [8, 512, 2048], P('ep')
- output 4: float32 [8, 2048, 512], P('ep')
- output 5: float32 [512, 8], replicated
All inputs are finite; a program needn't handle non-finite values.
Results may differ from the reference program's by a relative error of at most 0.00501279.
Values are sent between devices in bfloat16 or wider.
A program may use at most 1 GiB of HBM per device.

```python
import jax
import jax.numpy as jnp
from jax import lax

EXPERTS = 8
TOKENS_DEV = 512
D_MODEL = 512
D_HIDDEN = 2048
HOT_EXPERTS = 3

CAP_ROWS = TOKENS_DEV // 4
ALL_TOKENS = EXPERTS * TOKENS_DEV
CAP_ALL = EXPERTS * CAP_ROWS


def draw_routes(route_key):
    k_perm, k_shift, k_order, k_swap = jax.random.split(route_key, 4)
    n_cold = EXPERTS - HOT_EXPERTS
    cold_choices = 2 * TOKENS_DEV - HOT_EXPERTS * CAP_ROWS
    slot_pos = jnp.arange(2 * TOKENS_DEV)
    hot_rank = jnp.minimum(slot_pos // CAP_ROWS, HOT_EXPERTS - 1)
    cold_block = (jnp.maximum(slot_pos - HOT_EXPERTS * CAP_ROWS, 0) * n_cold) // cold_choices
    shifts = jax.random.randint(k_shift, (EXPERTS, 1), 0, n_cold)
    cold_rank = HOT_EXPERTS + (cold_block[None, :] + shifts) % n_cold
    rank_ids = jnp.where(slot_pos[None, :] < HOT_EXPERTS * CAP_ROWS, hot_rank[None, :], cold_rank)
    expert_perm = jax.random.permutation(k_perm, EXPERTS)
    choice_ids = expert_perm[rank_ids]
    pair_ids = jnp.stack([choice_ids[:, :TOKENS_DEV], choice_ids[:, TOKENS_DEV:]], axis=-1)
    token_perm = jax.random.permutation(k_order, jnp.tile(jnp.arange(TOKENS_DEV), (EXPERTS, 1)), axis=1, independent=True)
    pair_ids = jnp.take_along_axis(pair_ids, token_perm[:, :, None], axis=1)
    swap_bit = jax.random.randint(k_swap, (EXPERTS, TOKENS_DEV, 1), 0, 2)
    pair_ids = jnp.where(swap_bit == 1, pair_ids[:, :, ::-1], pair_ids)
    return pair_ids.reshape(ALL_TOKENS, 2).astype(jnp.int32)


def setup_inputs(seed: int = 0) -> dict:
    rng_key = jax.random.key(seed)
    k_tok, k_grad, k_route, k_gate, k_in, k_out = jax.random.split(rng_key, 6)
    tokens = jax.random.normal(k_tok, (ALL_TOKENS, D_MODEL), jnp.float32).astype(jnp.bfloat16)
    grad_out = jax.random.normal(k_grad, (ALL_TOKENS, D_MODEL), jnp.float32).astype(jnp.bfloat16)
    expert_ids = draw_routes(k_route)
    w_gate = (jax.random.normal(k_gate, (D_MODEL, EXPERTS), jnp.float32) * D_MODEL ** -0.5).astype(jnp.bfloat16)
    w_in = (jax.random.normal(k_in, (EXPERTS, D_MODEL, D_HIDDEN), jnp.float32) * D_MODEL ** -0.5).astype(jnp.bfloat16)
    w_out = (jax.random.normal(k_out, (EXPERTS, D_HIDDEN, D_MODEL), jnp.float32) * D_HIDDEN ** -0.5).astype(jnp.bfloat16)
    return {'tokens': tokens, 'grad_out': grad_out, 'expert_ids': expert_ids, 'w_gate': w_gate, 'w_in': w_in, 'w_out': w_out}


def reference(tokens, grad_out, expert_ids, w_gate, w_in, w_out):
    n_choice = 2 * ALL_TOKENS
    logits = jnp.dot(tokens, w_gate, preferred_element_type=jnp.float32)
    prob_all = jax.nn.softmax(logits, axis=-1)
    picked = jnp.take_along_axis(prob_all, expert_ids, axis=1)
    gate_val = picked / jnp.sum(picked, axis=1, keepdims=True)
    flat_ids = expert_ids.reshape(-1)
    sort_order = jnp.argsort(flat_ids, stable=True)
    counts = jnp.bincount(flat_ids, length=EXPERTS)
    starts = jnp.cumsum(counts) - counts
    pad_rows = jnp.zeros((CAP_ALL, D_MODEL), jnp.bfloat16)
    x_sorted = jnp.concatenate([tokens[sort_order // 2], pad_rows], axis=0)
    dy_flat = (gate_val[:, :, None] * grad_out[:, None, :].astype(jnp.float32)).astype(jnp.bfloat16).reshape(n_choice, D_MODEL)
    dy_sorted = jnp.concatenate([dy_flat[sort_order], pad_rows], axis=0)
    row_iota = jnp.arange(CAP_ALL)[:, None]

    def expert_step(scan_carry, per_expert):
        y_acc, dx_acc = scan_carry
        w_one, w_two, start_row, row_count = per_expert
        keep_row = row_iota < row_count
        x_rows = jnp.where(keep_row, lax.dynamic_slice_in_dim(x_sorted, start_row, CAP_ALL), 0)
        dy_rows = jnp.where(keep_row, lax.dynamic_slice_in_dim(dy_sorted, start_row, CAP_ALL), 0)
        a_pre = jnp.dot(x_rows, w_one, preferred_element_type=jnp.float32)
        hidden, gelu_vjp = jax.vjp(jax.nn.gelu, a_pre)
        hid_b = hidden.astype(jnp.bfloat16)
        y_rows = jnp.dot(hid_b, w_two, preferred_element_type=jnp.float32).astype(jnp.bfloat16)
        g_two = jnp.dot(hid_b.T, dy_rows, preferred_element_type=jnp.float32)
        d_hid = jnp.dot(dy_rows, w_two.T, preferred_element_type=jnp.float32)
        d_pre = gelu_vjp(d_hid)[0].astype(jnp.bfloat16)
        g_one = jnp.dot(x_rows.T, d_pre, preferred_element_type=jnp.float32)
        dx_rows = jnp.dot(d_pre, w_one.T, preferred_element_type=jnp.float32).astype(jnp.bfloat16)
        y_acc = lax.dynamic_update_slice_in_dim(y_acc, lax.dynamic_slice_in_dim(y_acc, start_row, CAP_ALL) + y_rows.astype(jnp.float32), start_row, axis=0)
        dx_acc = lax.dynamic_update_slice_in_dim(dx_acc, lax.dynamic_slice_in_dim(dx_acc, start_row, CAP_ALL) + dx_rows.astype(jnp.float32), start_row, axis=0)
        return (y_acc, dx_acc), (g_one, g_two)

    acc_init = jnp.zeros((n_choice + CAP_ALL, D_MODEL), jnp.float32)
    acc_done, grads = lax.scan(expert_step, (acc_init, acc_init), (w_in, w_out, starts, counts))
    g_in, g_out = grads
    y_sorted = acc_done[0][:n_choice]
    dx_sorted = acc_done[1][:n_choice]
    y_pair = jnp.zeros_like(y_sorted).at[sort_order].set(y_sorted).reshape(ALL_TOKENS, 2, D_MODEL)
    dx_pair = jnp.zeros_like(dx_sorted).at[sort_order].set(dx_sorted).reshape(ALL_TOKENS, 2, D_MODEL)
    y_out = jnp.sum(gate_val[:, :, None] * y_pair, axis=1).astype(jnp.bfloat16)
    d_gate = jnp.sum(grad_out.astype(jnp.float32)[:, None, :] * y_pair, axis=-1)
    d_sel = gate_val * (d_gate - jnp.sum(gate_val * d_gate, axis=1, keepdims=True))
    choice_hot = expert_ids[:, :, None] == jnp.arange(EXPERTS)[None, None, :]
    d_logits = jnp.sum(jnp.where(choice_hot, d_sel[:, :, None], 0.0), axis=1).astype(jnp.bfloat16)
    grad_x = (jnp.sum(dx_pair, axis=1) + jnp.dot(d_logits, w_gate.T, preferred_element_type=jnp.float32)).astype(jnp.bfloat16)
    grad_w_gate = jnp.dot(tokens.T, d_logits, preferred_element_type=jnp.float32)
    return y_out, grad_x, g_in, g_out, grad_w_gate
```

```python
import functools

import jax
import jax.numpy as jnp
from jax import lax
from jax.experimental import pallas as pl
from jax.experimental.pallas import tpu as pltpu
from jax.sharding import PartitionSpec as P

N_DEV = 8
ROWS = 128
MESH = pl.DeviceIdType.MESH
F32 = jnp.float32
BF16 = jnp.bfloat16
SQRT_2_PI = 0.7978845608028654
CUBIC = 0.044715


def dot_nn(a, b):
    return lax.dot_general(a, b, (((1,), (0,)), ((), ())), preferred_element_type=F32)


def dot_nt(a, b):
    return lax.dot_general(a, b, (((1,), (1,)), ((), ())), preferred_element_type=F32)


def dot_tn(a, b):
    return lax.dot_general(a, b, (((0,), (0,)), ((), ())), preferred_element_type=F32)


def moe_kernel(ids_ref, wgt_ref, x_hbm, dout_hbm, win_hbm, wout_hbm,
               out_ref, gx_ref, gwin_ref, gwout_ref, gwg_ref,
               x_v, dout_v, win_v, wout_v, rank_v, p_v, q0_v, q1_v, dyflat_v, gate_v, cols_v,
               sx, rx, sdy, rdy, sy, ry, sdx, rdx, h_v, gp_v, da_v, xt_v, wg_part, wg_all,
               load_sem, send_sem, recv_sem, wg_send, wg_recv):
    tok = x_v.shape[0]
    d_hid = win_v.shape[1]
    me = lax.axis_index('ep')
    core, col, row = me % 2, (me // 2) % 2, me // 4

    def peer(d):
        return 4 * ((row + d // 4) % 2) + 2 * ((col + (d // 2) % 2) % 2) + (core + d % 2) % 2

    def remote(phase, src, dst, d):
        return pltpu.make_async_remote_copy(
            src_ref=src.at[pl.ds(d * ROWS, ROWS)], dst_ref=dst.at[pl.ds(d * ROWS, ROWS)], send_sem=send_sem.at[phase, d], recv_sem=recv_sem.at[phase, d],
            device_id=(peer(d),), device_id_type=MESH)

    barrier = pltpu.get_barrier_semaphore()
    for d in range(1, N_DEV):
        pl.semaphore_signal(barrier, inc=1, device_id=(peer(d),), device_id_type=MESH)
    loads = [pltpu.make_async_copy(src, dst, load_sem.at[i]) for i, (src, dst) in enumerate(
        ((x_hbm, x_v), (dout_hbm, dout_v), (win_hbm, win_v), (wout_hbm, wout_v)))]
    for ld in loads:
        ld.start()

    rel = lax.broadcasted_iota(jnp.int32, (16, tok), 0) ^ me
    ids0 = ids_ref[0:1, :]
    ids1 = ids_ref[1:2, :]
    hit0 = rel == ids0
    hit1 = rel == ids1
    hot = jnp.where(hit0 | hit1, 1.0, 0.0).astype(BF16)
    before = jnp.where(lax.broadcasted_iota(jnp.int32, (tok, tok), 0) < lax.broadcasted_iota(jnp.int32, (tok, tok), 1), 1.0, 0.0).astype(BF16)
    rank = dot_nn(hot, before)
    rank0 = jnp.where(hit0, rank, -1.0)
    rank1 = jnp.where(hit1, rank, -1.0)
    rank_v[0:16, :] = rank0
    rank_v[16:32, :] = rank1
    slot = lax.broadcasted_iota(jnp.int32, (ROWS, tok), 0).astype(F32)

    loads[0].wait()
    pl.semaphore_wait(barrier, N_DEV - 1)
    for d in (2, 4, 3, 5, 6, 7, 1, 0):
        pick0 = jnp.where(rank_v[d:d + 1, :] == slot, 1.0, 0.0)
        pick1 = jnp.where(rank_v[16 + d:17 + d, :] == slot, 1.0, 0.0)
        block = dot_nn((pick0 + pick1).astype(BF16), x_v[...]).astype(BF16)
        if d == 0:
            rx[0:ROWS] = block
        else:
            sx[d * ROWS:(d + 1) * ROWS] = block
            remote(0, sx, rx, d).start()
        p_v[d, :, 0:tok] = pick0.astype(BF16)
        p_v[d, :, tok:2 * tok] = pick1.astype(BF16)

    stack = jnp.concatenate([rank0, rank1, jnp.broadcast_to(ids0.astype(F32), (16, tok)),
                             jnp.broadcast_to(ids1.astype(F32), (16, tok)), jnp.zeros((64, tok), F32)], axis=0)
    cols_v[...] = stack.T
    logits = dot_nt(x_v[...], wgt_ref[...])
    lane8 = lax.broadcasted_iota(jnp.int32, (tok, N_DEV), 1).astype(F32)
    sel0 = jnp.sum(jnp.where(lane8 == cols_v[:, 32:33], logits, 0.0), axis=1, keepdims=True)
    sel1 = jnp.sum(jnp.where(lane8 == cols_v[:, 48:49], logits, 0.0), axis=1, keepdims=True)
    top = jnp.maximum(sel0, sel1)
    e0 = jnp.exp(sel0 - top)
    e1 = jnp.exp(sel1 - top)
    gate_v[0] = e0 / (e0 + e1)
    gate_v[1] = e1 / (e0 + e1)
    loads[1].wait()
    dout_f = dout_v[...].astype(F32)
    dyflat_v[0:tok, :] = (gate_v[0] * dout_f).astype(BF16)
    dyflat_v[tok:2 * tok, :] = (gate_v[1] * dout_f).astype(BF16)
    for d in (2, 4, 3, 5, 6, 7, 1, 0):
        block = dot_nn(p_v[d], dyflat_v[...]).astype(BF16)
        if d == 0:
            rdy[0:ROWS] = block
        else:
            sdy[d * ROWS:(d + 1) * ROWS] = block
            remote(1, sdy, rdy, d).start()

    hid = 512
    loads[2].wait()
    loads[3].wait()
    for c in range(4):
        for d in (2 * c, 2 * c + 1):
            if d:
                remote(0, sx, rx, d).wait_recv()
        rows = slice(2 * ROWS * c, 2 * ROWS * (c + 1))
        x_c = rx[rows]

        def fwd_tile(j, carry):
            cols = pl.ds(pl.multiple_of(j * hid, hid), hid)
            a = dot_nn(x_c, win_v[:, cols])
            sq = a * a
            t = jnp.tanh(SQRT_2_PI * (a + CUBIC * (a * sq)))
            cdf = 0.5 * (1.0 + t)
            h_v[rows, cols] = (a * cdf).astype(BF16)
            gp_v[rows, cols] = cdf + (0.5 * a) * (1.0 - t * t) * (SQRT_2_PI * (1.0 + (3.0 * CUBIC) * sq))
            return carry

        lax.fori_loop(0, d_hid // hid, fwd_tile, 0)
        y_c = dot_nn(h_v[rows, :], wout_v[...]).astype(BF16)
        for i, d in enumerate((2 * c, 2 * c + 1)):
            block = y_c[i * ROWS:(i + 1) * ROWS]
            if d == 0:
                ry[0:ROWS] = block
            else:
                sy[d * ROWS:(d + 1) * ROWS] = block
                remote(2, sy, ry, d).start()

    slot_l = lax.broadcasted_iota(jnp.int32, (tok, ROWS), 1).astype(F32)
    for d in range(N_DEV):
        q0_v[:, d * ROWS:(d + 1) * ROWS] = jnp.where(cols_v[:, d:d + 1] == slot_l, 1.0, 0.0).astype(BF16)
        q1_v[:, d * ROWS:(d + 1) * ROWS] = jnp.where(cols_v[:, 16 + d:17 + d] == slot_l, 1.0, 0.0).astype(BF16)

    def bwd_chunk(c):
        for d in (2 * c, 2 * c + 1):
            if d:
                remote(1, sdy, rdy, d).wait_recv()
        rows = slice(2 * ROWS * c, 2 * ROWS * (c + 1))
        dy_c = rdy[rows]

        def bwd_tile(j, carry):
            cols = pl.ds(pl.multiple_of(j * hid, hid), hid)
            dh = dot_nt(dy_c, wout_v[cols, :])
            da_v[rows, cols] = (dh * gp_v[rows, cols]).astype(BF16)
            return carry

        lax.fori_loop(0, d_hid // hid, bwd_tile, 0)
        dx_c = dot_nt(da_v[rows, :], win_v[...]).astype(BF16)
        for i, d in enumerate((2 * c, 2 * c + 1)):
            block = dx_c[i * ROWS:(i + 1) * ROWS]
            if d == 0:
                rdx[0:ROWS] = block
            else:
                sdx[d * ROWS:(d + 1) * ROWS] = block
                if c < 3:
                    remote(3, sdx, rdx, d).start()

    for c in range(4):
        bwd_chunk(c)

    xt_v[...] = rx[...].T
    wt = 256

    def grad_tile(j, carry):
        cols = pl.ds(pl.multiple_of(j * wt, wt), wt)
        gwout_ref[cols, :] = dot_tn(h_v[:, cols], rdy[...])
        gwin_ref[:, cols] = dot_nn(xt_v[...], da_v[:, cols])
        return carry

    lax.fori_loop(0, d_hid // wt, grad_tile, 0)

    for d in range(1, N_DEV):
        remote(2, sy, ry, d).wait_recv()
    y0 = dot_nn(q0_v[...], ry[...])
    y1 = dot_nn(q1_v[...], ry[...])
    g0 = gate_v[0]
    g1 = gate_v[1]
    dout_f = dout_v[...].astype(F32)
    out_ref[...] = (g0 * y0 + g1 * y1).astype(BF16)
    dg0 = jnp.sum(dout_f * y0, axis=1, keepdims=True)
    dg1 = jnp.sum(dout_f * y1, axis=1, keepdims=True)
    mean = g0 * dg0 + g1 * dg1
    d_log = (jnp.where(lane8 == cols_v[:, 32:33], g0 * (dg0 - mean), 0.0)
             + jnp.where(lane8 == cols_v[:, 48:49], g1 * (dg1 - mean), 0.0)).astype(BF16)
    wg_part[...] = dot_tn(d_log, x_v[...])
    wg_all[me] = wg_part[...]

    def wg_copy(d):
        return pltpu.make_async_remote_copy(
            src_ref=wg_part, dst_ref=wg_all.at[me], send_sem=wg_send.at[d], recv_sem=wg_recv.at[d],
            device_id=(peer(d),), device_id_type=MESH)

    for d in range(1, N_DEV):
        wg_copy(d).start()
    for d in (6, 7):
        remote(3, sdx, rdx, d).start()
    acc = dot_nn(d_log, wgt_ref[...])

    for c in range(4):
        for d in (2 * c, 2 * c + 1):
            if d:
                remote(3, sdx, rdx, d).wait_recv()
        span = slice(2 * ROWS * c, 2 * ROWS * (c + 1))
        acc = acc + dot_nn(q0_v[:, span] + q1_v[:, span], rdx[span])
    gx_ref[...] = acc.astype(BF16)
    for d in range(1, N_DEV):
        wg_copy(d).wait_recv()
    total = wg_all[0]
    for s in range(1, N_DEV):
        total = total + wg_all[s]
    gwg_ref[...] = total
    for d in range(1, N_DEV):
        remote(0, sx, rx, d).wait_send()
        remote(1, sdy, rdy, d).wait_send()
        remote(2, sy, ry, d).wait_send()
        remote(3, sdx, rdx, d).wait_send()
        wg_copy(d).wait_send()


def local_block(tokens, grad_out, expert_ids, w_gate, w_in, w_out):
    tok, d_model = tokens.shape
    n_exp = w_gate.shape[1]
    d_hid = w_in.shape[2]
    slots = n_exp * ROWS
    vmem = pl.BlockSpec(memory_space=pltpu.VMEM)
    hbm = pl.BlockSpec(memory_space=pl.ANY)
    blocks = pltpu.VMEM((slots, d_model), BF16)
    out, gx, gwin, gwout, gwg = pl.pallas_call(
        moe_kernel,
        out_shape=(jax.ShapeDtypeStruct((tok, d_model), BF16), jax.ShapeDtypeStruct((tok, d_model), BF16),
                   jax.ShapeDtypeStruct((d_model, d_hid), F32), jax.ShapeDtypeStruct((d_hid, d_model), F32),
                   jax.ShapeDtypeStruct((n_exp, d_model), F32)),
        in_specs=[vmem, vmem, hbm, hbm, hbm, hbm],
        out_specs=(vmem,) * 5,
        scratch_shapes=[
            pltpu.VMEM((tok, d_model), BF16), pltpu.VMEM((tok, d_model), BF16),
            pltpu.VMEM((d_model, d_hid), BF16), pltpu.VMEM((d_hid, d_model), BF16),
            pltpu.VMEM((32, tok), F32), pltpu.VMEM((n_exp, ROWS, 2 * tok), BF16),
            pltpu.VMEM((tok, slots), BF16), pltpu.VMEM((tok, slots), BF16),
            pltpu.VMEM((2 * tok, d_model), BF16), pltpu.VMEM((2, tok, 1), F32), pltpu.VMEM((tok, 128), F32),
            blocks, blocks, blocks, blocks, blocks, blocks, blocks, blocks,
            pltpu.VMEM((slots, d_hid), BF16), pltpu.VMEM((slots, d_hid), F32), pltpu.VMEM((slots, d_hid), BF16),
            pltpu.VMEM((d_model, slots), BF16), pltpu.VMEM((n_exp, d_model), F32), pltpu.VMEM((n_exp, n_exp, d_model), F32),
            pltpu.SemaphoreType.DMA((4,)), pltpu.SemaphoreType.DMA((4, n_exp)), pltpu.SemaphoreType.DMA((4, n_exp)),
            pltpu.SemaphoreType.DMA((n_exp,)), pltpu.SemaphoreType.DMA((n_exp,)),
        ],
        compiler_params=pltpu.CompilerParams(collective_id=0, has_side_effects=True, vmem_limit_bytes=47 * 1024 * 1024),
        name='moe_step',
    )(expert_ids.T, w_gate.T, tokens, grad_out, w_in[0], w_out[0])
    return out, gx, gwin[None], gwout[None], gwg.T


def solution(mesh):
    return jax.shard_map(local_block, mesh=mesh, in_specs=(P('ep'), P('ep'), P('ep'), P(), P('ep'), P('ep')), out_specs=(P('ep'), P('ep'), P('ep'), P('ep'), P()), check_vma=False)
```

```python
import functools

import jax
import jax.numpy as jnp
from jax import lax
from jax.experimental import pallas as pl
from jax.experimental.pallas import tpu as pltpu
from jax.sharding import PartitionSpec as P

N_DEV = 8
ROWS = 128
MESH = pl.DeviceIdType.MESH
F32 = jnp.float32
BF16 = jnp.bfloat16
SQRT_2_PI = 0.7978845608028654
CUBIC = 0.044715


def dot_nn(a, b):
    return lax.dot_general(a, b, (((1,), (0,)), ((), ())), preferred_element_type=F32)


def dot_nt(a, b):
    return lax.dot_general(a, b, (((1,), (1,)), ((), ())), preferred_element_type=F32)


def dot_tn(a, b):
    return lax.dot_general(a, b, (((0,), (0,)), ((), ())), preferred_element_type=F32)


def moe_kernel(ids_hbm, wgt_hbm, x_hbm, dout_hbm, win_hbm, wout_hbm,
               out_ref, gwin_ref, gwout_ref, gwg_ref, acc_ref, qlast_ref, rdx,
               ids_ref, wgt_ref, x_v, dout_v, win_v, wout_v, rank_v, p_v, q0_v, q1_v, dyflat_v, gate_v, cols_v,
               sx, rx, sdy, rdy, sy, ry, sdx, h_v, gp_v, da_v, xt_v, wg_part, wg_all,
               load_sem, send_sem, recv_sem, wg_send, wg_recv):
    tok = x_v.shape[0]
    d_hid = win_v.shape[1]
    me = lax.axis_index('ep')
    core, col, row = me % 2, (me // 2) % 2, me // 4

    def peer(d):
        return 4 * ((row + d // 4) % 2) + 2 * ((col + (d // 2) % 2) % 2) + (core + d % 2) % 2

    def remote(phase, src, dst, d):
        return pltpu.make_async_remote_copy(
            src_ref=src.at[pl.ds(d * ROWS, ROWS)], dst_ref=dst.at[pl.ds(d * ROWS, ROWS)], send_sem=send_sem.at[phase, d], recv_sem=recv_sem.at[phase, d],
            device_id=(peer(d),), device_id_type=MESH)

    barrier = pltpu.get_barrier_semaphore()
    for d in range(1, N_DEV):
        pl.semaphore_signal(barrier, inc=1, device_id=(peer(d),), device_id_type=MESH)
    loads = [pltpu.make_async_copy(src, dst, load_sem.at[i]) for i, (src, dst) in enumerate(
        ((ids_hbm, ids_ref), (x_hbm, x_v), (wgt_hbm, wgt_ref), (dout_hbm, dout_v), (win_hbm, win_v), (wout_hbm, wout_v)))]
    for ld in loads:
        ld.start()

    rel = lax.broadcasted_iota(jnp.int32, (16, tok), 0) ^ me
    loads[0].wait()
    ids0 = ids_ref[0:1, :]
    ids1 = ids_ref[1:2, :]
    hit0 = rel == ids0
    hit1 = rel == ids1
    hot = jnp.where(hit0 | hit1, 1.0, 0.0).astype(BF16)
    before = jnp.where(lax.broadcasted_iota(jnp.int32, (tok, tok), 0) < lax.broadcasted_iota(jnp.int32, (tok, tok), 1), 1.0, 0.0).astype(BF16)
    rank = dot_nn(hot, before)
    rank0 = jnp.where(hit0, rank, -1.0)
    rank1 = jnp.where(hit1, rank, -1.0)
    rank_v[0:16, :] = rank0
    rank_v[16:32, :] = rank1
    slot = lax.broadcasted_iota(jnp.int32, (ROWS, tok), 0).astype(F32)

    loads[1].wait()
    pl.semaphore_wait(barrier, N_DEV - 1)
    for d in (2, 4, 3, 5, 6, 7, 1, 0):
        pick0 = jnp.where(rank_v[d:d + 1, :] == slot, 1.0, 0.0)
        pick1 = jnp.where(rank_v[16 + d:17 + d, :] == slot, 1.0, 0.0)
        block = dot_nn((pick0 + pick1).astype(BF16), x_v[...]).astype(BF16)
        if d == 0:
            rx[0:ROWS] = block
        else:
            sx[d * ROWS:(d + 1) * ROWS] = block
            remote(0, sx, rx, d).start()
        p_v[d, :, 0:tok] = pick0.astype(BF16)
        p_v[d, :, tok:2 * tok] = pick1.astype(BF16)

    stack = jnp.concatenate([rank0, rank1, jnp.broadcast_to(ids0.astype(F32), (16, tok)),
                             jnp.broadcast_to(ids1.astype(F32), (16, tok)), jnp.zeros((64, tok), F32)], axis=0)
    cols_v[...] = stack.T
    loads[2].wait()
    logits = dot_nt(x_v[...], wgt_ref[...])
    lane8 = lax.broadcasted_iota(jnp.int32, (tok, N_DEV), 1).astype(F32)
    sel0 = jnp.sum(jnp.where(lane8 == cols_v[:, 32:33], logits, 0.0), axis=1, keepdims=True)
    sel1 = jnp.sum(jnp.where(lane8 == cols_v[:, 48:49], logits, 0.0), axis=1, keepdims=True)
    top = jnp.maximum(sel0, sel1)
    e0 = jnp.exp(sel0 - top)
    e1 = jnp.exp(sel1 - top)
    gate_v[0] = e0 / (e0 + e1)
    gate_v[1] = e1 / (e0 + e1)
    loads[3].wait()
    dout_f = dout_v[...].astype(F32)
    dyflat_v[0:tok, :] = (gate_v[0] * dout_f).astype(BF16)
    dyflat_v[tok:2 * tok, :] = (gate_v[1] * dout_f).astype(BF16)
    for d in (2, 4, 3, 5, 6, 7, 1, 0):
        block = dot_nn(p_v[d], dyflat_v[...]).astype(BF16)
        if d == 0:
            rdy[0:ROWS] = block
        else:
            sdy[d * ROWS:(d + 1) * ROWS] = block
            remote(1, sdy, rdy, d).start()

    hid = 512
    loads[4].wait()
    loads[5].wait()
    for c in range(4):
        for d in (2 * c, 2 * c + 1):
            if d:
                remote(0, sx, rx, d).wait_recv()
        rows = slice(2 * ROWS * c, 2 * ROWS * (c + 1))
        x_c = rx[rows]

        def fwd_tile(j, carry):
            cols = pl.ds(pl.multiple_of(j * hid, hid), hid)
            a = dot_nn(x_c, win_v[:, cols])
            sq = a * a
            t = jnp.tanh(SQRT_2_PI * (a + CUBIC * (a * sq)))
            cdf = 0.5 * (1.0 + t)
            h_v[rows, cols] = (a * cdf).astype(BF16)
            gp_v[rows, cols] = cdf + (0.5 * a) * (1.0 - t * t) * (SQRT_2_PI * (1.0 + (3.0 * CUBIC) * sq))
            return carry

        lax.fori_loop(0, d_hid // hid, fwd_tile, 0)
        y_c = dot_nn(h_v[rows, :], wout_v[...]).astype(BF16)
        for i, d in enumerate((2 * c, 2 * c + 1)):
            block = y_c[i * ROWS:(i + 1) * ROWS]
            if d == 0:
                ry[0:ROWS] = block
            else:
                sy[d * ROWS:(d + 1) * ROWS] = block
                remote(2, sy, ry, d).start()

    slot_l = lax.broadcasted_iota(jnp.int32, (tok, ROWS), 1).astype(F32)
    for d in range(N_DEV):
        q0_v[:, d * ROWS:(d + 1) * ROWS] = jnp.where(cols_v[:, d:d + 1] == slot_l, 1.0, 0.0).astype(BF16)
        q1_v[:, d * ROWS:(d + 1) * ROWS] = jnp.where(cols_v[:, 16 + d:17 + d] == slot_l, 1.0, 0.0).astype(BF16)

    def bwd_chunk(c):
        for d in (2 * c, 2 * c + 1):
            if d:
                remote(1, sdy, rdy, d).wait_recv()
        rows = slice(2 * ROWS * c, 2 * ROWS * (c + 1))
        dy_c = rdy[rows]

        def bwd_tile(j, carry):
            cols = pl.ds(pl.multiple_of(j * hid, hid), hid)
            dh = dot_nt(dy_c, wout_v[cols, :])
            da_v[rows, cols] = (dh * gp_v[rows, cols]).astype(BF16)
            return carry

        lax.fori_loop(0, d_hid // hid, bwd_tile, 0)
        dx_c = dot_nt(da_v[rows, :], win_v[...]).astype(BF16)
        for i, d in enumerate((2 * c, 2 * c + 1)):
            block = dx_c[i * ROWS:(i + 1) * ROWS]
            if d == 0:
                rdx[0:ROWS] = block
            else:
                sdx[d * ROWS:(d + 1) * ROWS] = block
                if c < 3:
                    remote(3, sdx, rdx, d).start()

    for c in range(4):
        bwd_chunk(c)

    xt_v[...] = rx[...].T
    wt = 256

    def grad_tile(j, carry):
        cols = pl.ds(pl.multiple_of(j * wt, wt), wt)
        gwout_ref[cols, :] = dot_tn(h_v[:, cols], rdy[...])
        gwin_ref[:, cols] = dot_nn(xt_v[...], da_v[:, cols])
        return carry

    lax.fori_loop(0, d_hid // wt, grad_tile, 0)

    for d in range(1, N_DEV):
        remote(2, sy, ry, d).wait_recv()
    y0 = dot_nn(q0_v[...], ry[...])
    y1 = dot_nn(q1_v[...], ry[...])
    g0 = gate_v[0]
    g1 = gate_v[1]
    dout_f = dout_v[...].astype(F32)
    out_ref[...] = (g0 * y0 + g1 * y1).astype(BF16)
    dg0 = jnp.sum(dout_f * y0, axis=1, keepdims=True)
    dg1 = jnp.sum(dout_f * y1, axis=1, keepdims=True)
    mean = g0 * dg0 + g1 * dg1
    d_log = (jnp.where(lane8 == cols_v[:, 32:33], g0 * (dg0 - mean), 0.0)
             + jnp.where(lane8 == cols_v[:, 48:49], g1 * (dg1 - mean), 0.0)).astype(BF16)
    wg_part[...] = dot_tn(d_log, x_v[...])
    wg_all[me] = wg_part[...]

    def wg_copy(d):
        return pltpu.make_async_remote_copy(
            src_ref=wg_part, dst_ref=wg_all.at[me], send_sem=wg_send.at[d], recv_sem=wg_recv.at[d],
            device_id=(peer(d),), device_id_type=MESH)

    for d in range(1, N_DEV):
        wg_copy(d).start()
    for d in (6, 7):
        remote(3, sdx, rdx, d).start()
    acc = dot_nn(d_log, wgt_ref[...])

    for c in range(3):
        for d in (2 * c, 2 * c + 1):
            if d:
                remote(3, sdx, rdx, d).wait_recv()
        span = slice(2 * ROWS * c, 2 * ROWS * (c + 1))
        acc = acc + dot_nn(q0_v[:, span] + q1_v[:, span], rdx[span])
    acc_ref[...] = acc
    span = slice(6 * ROWS, 8 * ROWS)
    qlast_ref[...] = q0_v[:, span] + q1_v[:, span]
    for d in range(1, N_DEV):
        wg_copy(d).wait_recv()
    total = wg_all[0]
    for s in range(1, N_DEV):
        total = total + wg_all[s]
    gwg_ref[...] = total
    for d in (6, 7):
        remote(3, sdx, rdx, d).wait_recv()
    for d in range(1, N_DEV):
        remote(0, sx, rx, d).wait_send()
        remote(1, sdy, rdy, d).wait_send()
        remote(2, sy, ry, d).wait_send()
        remote(3, sdx, rdx, d).wait_send()
        wg_copy(d).wait_send()


def finish_kernel(out_v, gwin_v, gwout_v, gwg_v, acc_v, qlast_v, dx_v,
                  out_hbm, gx_hbm, gwin_hbm, gwout_hbm, gwg_hbm, gx_v, sem):
    stores = [pltpu.make_async_copy(src, dst, sem.at[i]) for i, (src, dst) in enumerate(
        ((gwin_v, gwin_hbm), (gwout_v, gwout_hbm), (out_v, out_hbm), (gwg_v, gwg_hbm), (gx_v, gx_hbm)))]
    for st in stores[:4]:
        st.start()
    gx_v[...] = (acc_v[...] + dot_nn(qlast_v[...], dx_v[6 * ROWS:8 * ROWS])).astype(BF16)
    stores[4].start()
    for st in stores:
        st.wait()


def local_block(tokens, grad_out, expert_ids, w_gate, w_in, w_out):
    tok, d_model = tokens.shape
    n_exp = w_gate.shape[1]
    d_hid = w_in.shape[2]
    slots = n_exp * ROWS
    vmem = pl.BlockSpec(memory_space=pltpu.VMEM)
    hbm = pl.BlockSpec(memory_space=pl.ANY)
    blocks = pltpu.VMEM((slots, d_model), BF16)
    args = [pltpu.with_memory_space_constraint(a, pltpu.HBM)
            for a in (expert_ids.T, w_gate.T, tokens, grad_out, w_in[0], w_out[0])]
    kept = pl.pallas_call(
        moe_kernel,
        out_shape=(pltpu.VMEM((tok, d_model), BF16), pltpu.VMEM((d_model, d_hid), F32), pltpu.VMEM((d_hid, d_model), F32),
                   pltpu.VMEM((n_exp, d_model), F32), pltpu.VMEM((tok, d_model), F32),
                   pltpu.VMEM((tok, 2 * ROWS), BF16), pltpu.VMEM((slots, d_model), BF16)),
        in_specs=[hbm] * 6,
        out_specs=(vmem,) * 7,
        scratch_shapes=[
            pltpu.VMEM((2, tok), jnp.int32), pltpu.VMEM((n_exp, d_model), BF16),
            pltpu.VMEM((tok, d_model), BF16), pltpu.VMEM((tok, d_model), BF16),
            pltpu.VMEM((d_model, d_hid), BF16), pltpu.VMEM((d_hid, d_model), BF16),
            pltpu.VMEM((32, tok), F32), pltpu.VMEM((n_exp, ROWS, 2 * tok), BF16),
            pltpu.VMEM((tok, slots), BF16), pltpu.VMEM((tok, slots), BF16),
            pltpu.VMEM((2 * tok, d_model), BF16), pltpu.VMEM((2, tok, 1), F32), pltpu.VMEM((tok, 128), F32),
            blocks, blocks, blocks, blocks, blocks, blocks, blocks,
            pltpu.VMEM((slots, d_hid), BF16), pltpu.VMEM((slots, d_hid), F32), pltpu.VMEM((slots, d_hid), BF16),
            pltpu.VMEM((d_model, slots), BF16), pltpu.VMEM((n_exp, d_model), F32), pltpu.VMEM((n_exp, n_exp, d_model), F32),
            pltpu.SemaphoreType.DMA((6,)), pltpu.SemaphoreType.DMA((4, n_exp)), pltpu.SemaphoreType.DMA((4, n_exp)),
            pltpu.SemaphoreType.DMA((n_exp,)), pltpu.SemaphoreType.DMA((n_exp,)),
        ],
        compiler_params=pltpu.CompilerParams(collective_id=0, has_side_effects=True, vmem_limit_bytes=46 * 1024 * 1024),
        name='moe_step',
    )(*args)
    out, gx, gwin, gwout, gwg = pl.pallas_call(
        finish_kernel,
        out_shape=(jax.ShapeDtypeStruct((tok, d_model), BF16), jax.ShapeDtypeStruct((tok, d_model), BF16),
                   jax.ShapeDtypeStruct((d_model, d_hid), F32), jax.ShapeDtypeStruct((d_hid, d_model), F32),
                   jax.ShapeDtypeStruct((n_exp, d_model), F32)),
        in_specs=[vmem] * 7,
        out_specs=(hbm,) * 5,
        scratch_shapes=[pltpu.VMEM((tok, d_model), BF16), pltpu.SemaphoreType.DMA((5,))],
        compiler_params=pltpu.CompilerParams(vmem_limit_bytes=16 * 1024 * 1024),
        name='moe_finish',
    )(*kept)
    return out, gx, gwin[None], gwout[None], gwg.T


def solution(mesh):
    return jax.shard_map(local_block, mesh=mesh, in_specs=(P('ep'), P('ep'), P('ep'), P(), P('ep'), P('ep')), out_specs=(P('ep'), P('ep'), P('ep'), P('ep'), P()), check_vma=False)
```

```python
import functools

import jax
import jax.numpy as jnp
from jax import lax
from jax.experimental import pallas as pl
from jax.experimental.pallas import tpu as pltpu
from jax.sharding import PartitionSpec as P

N_DEV = 8
ROWS = 128
MESH = pl.DeviceIdType.MESH
F32 = jnp.float32
BF16 = jnp.bfloat16
SQRT_2_PI = 0.7978845608028654
CUBIC = 0.044715


def dot_nn(a, b):
    return lax.dot_general(a, b, (((1,), (0,)), ((), ())), preferred_element_type=F32)


def dot_nt(a, b):
    return lax.dot_general(a, b, (((1,), (1,)), ((), ())), preferred_element_type=F32)


def dot_tn(a, b):
    return lax.dot_general(a, b, (((0,), (0,)), ((), ())), preferred_element_type=F32)


def moe_kernel(ids_hbm, wgt_hbm, x_hbm, dout_hbm, win_hbm, wout_hbm,
               out_ref, gwin_ref, gwout_ref, gwg_ref, acc_ref, qlast_ref, rdx,
               ids_ref, wgt_ref, x_v, dout_v, win_v, wout_v, rank_v, p_v, q0_v, q1_v, dyflat_v, gate_v, cols_v,
               sx, rx, sdy, rdy, sy, ry, sdx, h_v, gp_v, da_v, xt_v, before_v, wg_part, wg_mate, wg_chip,
               load_sem, send_sem, recv_sem, wg_send, wg_recv):
    tok = x_v.shape[0]
    d_hid = win_v.shape[1]
    half = x_v.shape[1] // 2
    me = lax.axis_index('ep')
    core, col, row = me % 2, (me // 2) % 2, me // 4

    def peer(d):
        return 4 * ((row + d // 4) % 2) + 2 * ((col + (d // 2) % 2) % 2) + (core + d % 2) % 2

    def remote(phase, src, dst, d):
        return pltpu.make_async_remote_copy(
            src_ref=src.at[pl.ds(d * ROWS, ROWS)], dst_ref=dst.at[pl.ds(d * ROWS, ROWS)], send_sem=send_sem.at[phase, d], recv_sem=recv_sem.at[phase, d],
            device_id=(peer(d),), device_id_type=MESH)

    barrier = pltpu.get_barrier_semaphore()
    for d in range(1, N_DEV):
        pl.semaphore_signal(barrier, inc=1, device_id=(peer(d),), device_id_type=MESH)
    loads = [pltpu.make_async_copy(src, dst, load_sem.at[i]) for i, (src, dst) in enumerate(
        ((ids_hbm, ids_ref), (x_hbm, x_v), (wgt_hbm, wgt_ref), (dout_hbm, dout_v), (win_hbm, win_v), (wout_hbm, wout_v)))]
    for ld in loads:
        ld.start()

    rel = lax.broadcasted_iota(jnp.int32, (16, tok), 0) ^ me
    before_v[...] = jnp.where(lax.broadcasted_iota(jnp.int32, (tok, tok), 0) < lax.broadcasted_iota(jnp.int32, (tok, tok), 1), 1.0, 0.0).astype(BF16)
    slot = lax.broadcasted_iota(jnp.int32, (ROWS, tok), 0).astype(F32)
    loads[0].wait()
    ids0 = ids_ref[0:1, :]
    ids1 = ids_ref[1:2, :]
    hit0 = rel == ids0
    hit1 = rel == ids1
    hot = jnp.where(hit0 | hit1, 1.0, 0.0).astype(BF16)
    rank = dot_nn(hot, before_v[...])
    rank0 = jnp.where(hit0, rank, -1.0)
    rank1 = jnp.where(hit1, rank, -1.0)
    rank_v[0:16, :] = rank0
    rank_v[16:32, :] = rank1

    loads[1].wait()
    for d in (2, 4, 3, 5, 6, 7, 1, 0):
        pick0 = jnp.where(rank_v[d:d + 1, :] == slot, 1.0, 0.0)
        pick1 = jnp.where(rank_v[16 + d:17 + d, :] == slot, 1.0, 0.0)
        block = dot_nn((pick0 + pick1).astype(BF16), x_v[...]).astype(BF16)
        if d == 0:
            rx[0:ROWS] = block
        else:
            sx[d * ROWS:(d + 1) * ROWS] = block
            if d == 2:
                pl.semaphore_wait(barrier, N_DEV - 1)
            remote(0, sx, rx, d).start()
        p_v[d, :, 0:tok] = pick0.astype(BF16)
        p_v[d, :, tok:2 * tok] = pick1.astype(BF16)

    stack = jnp.concatenate([rank0, rank1, jnp.broadcast_to(ids0.astype(F32), (16, tok)),
                             jnp.broadcast_to(ids1.astype(F32), (16, tok)), jnp.zeros((64, tok), F32)], axis=0)
    cols_v[...] = stack.T
    loads[2].wait()
    logits = dot_nt(x_v[...], wgt_ref[...])
    lane8 = lax.broadcasted_iota(jnp.int32, (tok, N_DEV), 1).astype(F32)
    sel0 = jnp.sum(jnp.where(lane8 == cols_v[:, 32:33], logits, 0.0), axis=1, keepdims=True)
    sel1 = jnp.sum(jnp.where(lane8 == cols_v[:, 48:49], logits, 0.0), axis=1, keepdims=True)
    top = jnp.maximum(sel0, sel1)
    e0 = jnp.exp(sel0 - top)
    e1 = jnp.exp(sel1 - top)
    gate_v[0] = e0 / (e0 + e1)
    gate_v[1] = e1 / (e0 + e1)
    loads[3].wait()
    dout_f = dout_v[...].astype(F32)
    dyflat_v[0:tok, :] = (gate_v[0] * dout_f).astype(BF16)
    dyflat_v[tok:2 * tok, :] = (gate_v[1] * dout_f).astype(BF16)
    for d in (2, 4, 3, 5, 6, 7, 1, 0):
        block = dot_nn(p_v[d], dyflat_v[...]).astype(BF16)
        if d == 0:
            rdy[0:ROWS] = block
        else:
            sdy[d * ROWS:(d + 1) * ROWS] = block
            remote(1, sdy, rdy, d).start()

    hid = 512
    loads[4].wait()
    loads[5].wait()
    for c in range(4):
        for d in (2 * c, 2 * c + 1):
            if d:
                remote(0, sx, rx, d).wait_recv()
        rows = slice(2 * ROWS * c, 2 * ROWS * (c + 1))
        x_c = rx[rows]

        def fwd_tile(j, carry):
            cols = pl.ds(pl.multiple_of(j * hid, hid), hid)
            a = dot_nn(x_c, win_v[:, cols])
            sq = a * a
            t = jnp.tanh(SQRT_2_PI * (a + CUBIC * (a * sq)))
            cdf = 0.5 * (1.0 + t)
            h_v[rows, cols] = (a * cdf).astype(BF16)
            gp_v[rows, cols] = cdf + (0.5 * a) * (1.0 - t * t) * (SQRT_2_PI * (1.0 + (3.0 * CUBIC) * sq))
            return carry

        lax.fori_loop(0, d_hid // hid, fwd_tile, 0)
        y_c = dot_nn(h_v[rows, :], wout_v[...]).astype(BF16)
        for i, d in enumerate((2 * c, 2 * c + 1)):
            block = y_c[i * ROWS:(i + 1) * ROWS]
            if d == 0:
                ry[0:ROWS] = block
            else:
                sy[d * ROWS:(d + 1) * ROWS] = block
                remote(2, sy, ry, d).start()

    slot_l = lax.broadcasted_iota(jnp.int32, (tok, ROWS), 1).astype(F32)
    for d in range(N_DEV):
        q0_v[:, d * ROWS:(d + 1) * ROWS] = jnp.where(cols_v[:, d:d + 1] == slot_l, 1.0, 0.0).astype(BF16)
        q1_v[:, d * ROWS:(d + 1) * ROWS] = jnp.where(cols_v[:, 16 + d:17 + d] == slot_l, 1.0, 0.0).astype(BF16)

    def bwd_chunk(c):
        for d in (2 * c, 2 * c + 1):
            if d:
                remote(1, sdy, rdy, d).wait_recv()
        rows = slice(2 * ROWS * c, 2 * ROWS * (c + 1))
        dy_c = rdy[rows]

        def bwd_tile(j, carry):
            cols = pl.ds(pl.multiple_of(j * hid, hid), hid)
            dh = dot_nt(dy_c, wout_v[cols, :])
            da_v[rows, cols] = (dh * gp_v[rows, cols]).astype(BF16)
            return carry

        lax.fori_loop(0, d_hid // hid, bwd_tile, 0)
        dx_c = dot_nt(da_v[rows, :], win_v[...]).astype(BF16)
        for i, d in enumerate((2 * c, 2 * c + 1)):
            block = dx_c[i * ROWS:(i + 1) * ROWS]
            if d == 0:
                rdx[0:ROWS] = block
            else:
                sdx[d * ROWS:(d + 1) * ROWS] = block
                if c in (0, 3):
                    remote(3, sdx, rdx, d).start()

    for c in range(4):
        bwd_chunk(c)

    xt_v[...] = rx[...].T
    wt = 256

    def grad_tile(j, carry):
        cols = pl.ds(pl.multiple_of(j * wt, wt), wt)
        gwout_ref[cols, :] = dot_tn(h_v[:, cols], rdy[...])
        gwin_ref[:, cols] = dot_nn(xt_v[...], da_v[:, cols])
        return carry

    lax.fori_loop(0, d_hid // wt, grad_tile, 0)

    for d in range(1, N_DEV):
        remote(2, sy, ry, d).wait_recv()
    y0 = dot_nn(q0_v[...], ry[...])
    y1 = dot_nn(q1_v[...], ry[...])
    g0 = gate_v[0]
    g1 = gate_v[1]
    dout_f = dout_v[...].astype(F32)
    out_ref[...] = (g0 * y0 + g1 * y1).astype(BF16)
    dg0 = jnp.sum(dout_f * y0, axis=1, keepdims=True)
    dg1 = jnp.sum(dout_f * y1, axis=1, keepdims=True)
    mean = g0 * dg0 + g1 * dg1
    d_log = (jnp.where(lane8 == cols_v[:, 32:33], g0 * (dg0 - mean), 0.0)
             + jnp.where(lane8 == cols_v[:, 48:49], g1 * (dg1 - mean), 0.0)).astype(BF16)
    for i in range(2):
        wg_part[i] = dot_tn(d_log, x_v[:, i * half:(i + 1) * half])

    def wg_copy(i, src, dst, d):
        return pltpu.make_async_remote_copy(
            src_ref=src, dst_ref=dst, send_sem=wg_send.at[i], recv_sem=wg_recv.at[i],
            device_id=(peer(d),), device_id_type=MESH)

    chip = 2 * row + col
    to_mate = wg_copy(0, wg_part.at[1 - core], wg_mate, 1)
    to_mate.start()
    acc = dot_nn(d_log, wgt_ref[...])
    to_mate.wait_recv()
    wg_chip[chip] = wg_part[core] + wg_mate[...]
    to_chips = [wg_copy(1 + i, wg_chip.at[chip], wg_chip.at[chip], 2 * (i + 1)) for i in range(3)]
    for cp in to_chips:
        cp.start()
    for d in (2, 4, 3, 5):
        remote(3, sdx, rdx, d).start()

    for c in (0, 3):
        for d in (2 * c, 2 * c + 1):
            if d:
                remote(3, sdx, rdx, d).wait_recv()
        span = slice(2 * ROWS * c, 2 * ROWS * (c + 1))
        acc = acc + dot_nn(q0_v[:, span] + q1_v[:, span], rdx[span])
    acc_ref[...] = acc
    span = slice(2 * ROWS, 6 * ROWS)
    qlast_ref[...] = q0_v[:, span] + q1_v[:, span]
    for cp in to_chips:
        cp.wait_recv()
    gwg_ref[core] = (wg_chip[0] + wg_chip[1]) + (wg_chip[2] + wg_chip[3])
    swap = wg_copy(4, gwg_ref.at[core], gwg_ref.at[core], 1)
    swap.start()
    to_mate.wait_send()
    for d in range(1, N_DEV):
        remote(0, sx, rx, d).wait_send()
        remote(1, sdy, rdy, d).wait_send()
        remote(2, sy, ry, d).wait_send()
    for cp in to_chips:
        cp.wait_send()
    swap.wait()
    for d in (2, 4, 3, 5):
        remote(3, sdx, rdx, d).wait_recv()
    for d in range(1, N_DEV):
        remote(3, sdx, rdx, d).wait_send()


def finish_kernel(out_v, gwin_v, gwout_v, gwg_v, acc_v, qlast_v, dx_v,
                  out_hbm, gx_hbm, gwin_hbm, gwout_hbm, gwg_hbm, gx_v, sem):
    pieces = []
    for src, dst in ((gwin_v, gwin_hbm), (gwout_v, gwout_hbm)):
        n = src.shape[0] // 4
        pieces += [(src.at[pl.ds(i * n, n)], dst.at[pl.ds(i * n, n)]) for i in range(4)]
    half = gwg_v.shape[2]
    pieces += [(out_v, out_hbm), (gwg_v.at[0], gwg_hbm.at[:, pl.ds(0, half)]), (gwg_v.at[1], gwg_hbm.at[:, pl.ds(half, half)]),
               (gx_v, gx_hbm)]
    stores = [pltpu.make_async_copy(src, dst, sem.at[i]) for i, (src, dst) in enumerate(pieces)]
    for st in stores[:-1]:
        st.start()
    gx_v[...] = (acc_v[...] + dot_nn(qlast_v[...], dx_v[2 * ROWS:6 * ROWS])).astype(BF16)
    stores[-1].start()
    for st in stores:
        st.wait()


def local_block(tokens, grad_out, expert_ids, w_gate, w_in, w_out):
    tok, d_model = tokens.shape
    n_exp = w_gate.shape[1]
    d_hid = w_in.shape[2]
    slots = n_exp * ROWS
    vmem = pl.BlockSpec(memory_space=pltpu.VMEM)
    hbm = pl.BlockSpec(memory_space=pl.ANY)
    blocks = pltpu.VMEM((slots, d_model), BF16)
    args = [pltpu.with_memory_space_constraint(a, pltpu.HBM)
            for a in (expert_ids.T, w_gate.T, tokens, grad_out, w_in[0], w_out[0])]
    kept = pl.pallas_call(
        moe_kernel,
        out_shape=(pltpu.VMEM((tok, d_model), BF16), pltpu.VMEM((d_model, d_hid), F32), pltpu.VMEM((d_hid, d_model), F32),
                   pltpu.VMEM((2, n_exp, d_model // 2), F32), pltpu.VMEM((tok, d_model), F32),
                   pltpu.VMEM((tok, 4 * ROWS), BF16), pltpu.VMEM((slots, d_model), BF16)),
        in_specs=[hbm] * 6,
        out_specs=(vmem,) * 7,
        scratch_shapes=[
            pltpu.VMEM((2, tok), jnp.int32), pltpu.VMEM((n_exp, d_model), BF16),
            pltpu.VMEM((tok, d_model), BF16), pltpu.VMEM((tok, d_model), BF16),
            pltpu.VMEM((d_model, d_hid), BF16), pltpu.VMEM((d_hid, d_model), BF16),
            pltpu.VMEM((32, tok), F32), pltpu.VMEM((n_exp, ROWS, 2 * tok), BF16),
            pltpu.VMEM((tok, slots), BF16), pltpu.VMEM((tok, slots), BF16),
            pltpu.VMEM((2 * tok, d_model), BF16), pltpu.VMEM((2, tok, 1), F32), pltpu.VMEM((tok, 128), F32),
            blocks, blocks, blocks, blocks, blocks, blocks, blocks,
            pltpu.VMEM((slots, d_hid), BF16), pltpu.VMEM((slots, d_hid), F32), pltpu.VMEM((slots, d_hid), BF16),
            pltpu.VMEM((d_model, slots), BF16), pltpu.VMEM((tok, tok), BF16),
            pltpu.VMEM((2, n_exp, d_model // 2), F32), pltpu.VMEM((n_exp, d_model // 2), F32), pltpu.VMEM((4, n_exp, d_model // 2), F32),
            pltpu.SemaphoreType.DMA((6,)), pltpu.SemaphoreType.DMA((4, n_exp)), pltpu.SemaphoreType.DMA((4, n_exp)),
            pltpu.SemaphoreType.DMA((5,)), pltpu.SemaphoreType.DMA((5,)),
        ],
        compiler_params=pltpu.CompilerParams(collective_id=0, has_side_effects=True, vmem_limit_bytes=46 * 1024 * 1024),
        name='moe_step',
    )(*args)
    out, gx, gwin, gwout, gwg = pl.pallas_call(
        finish_kernel,
        out_shape=(jax.ShapeDtypeStruct((tok, d_model), BF16), jax.ShapeDtypeStruct((tok, d_model), BF16),
                   jax.ShapeDtypeStruct((d_model, d_hid), F32), jax.ShapeDtypeStruct((d_hid, d_model), F32),
                   jax.ShapeDtypeStruct((n_exp, d_model), F32)),
        in_specs=[vmem] * 7,
        out_specs=(hbm,) * 5,
        scratch_shapes=[pltpu.VMEM((tok, d_model), BF16), pltpu.SemaphoreType.DMA((12,))],
        compiler_params=pltpu.CompilerParams(vmem_limit_bytes=16 * 1024 * 1024),
        name='moe_finish',
    )(*kept)
    return out, gx, gwin[None], gwout[None], gwg.T


def solution(mesh):
    return jax.shard_map(local_block, mesh=mesh, in_specs=(P('ep'), P('ep'), P('ep'), P(), P('ep'), P('ep')), out_specs=(P('ep'), P('ep'), P('ep'), P('ep'), P()), check_vma=False)
```

```python
import functools

import jax
import jax.numpy as jnp
from jax import lax
from jax.experimental import pallas as pl
from jax.experimental.pallas import tpu as pltpu
from jax.sharding import PartitionSpec as P

N_DEV = 8
DX_EARLY = (6, 2, 4, 7)
DX_LATE = (3, 5)
ROWS = 128
MESH = pl.DeviceIdType.MESH
F32 = jnp.float32
BF16 = jnp.bfloat16
SQRT_2_PI = 0.7978845608028654
CUBIC = 0.044715


def dot_nn(a, b):
    return lax.dot_general(a, b, (((1,), (0,)), ((), ())), preferred_element_type=F32)


def dot_nt(a, b):
    return lax.dot_general(a, b, (((1,), (1,)), ((), ())), preferred_element_type=F32)


def dot_tn(a, b):
    return lax.dot_general(a, b, (((0,), (0,)), ((), ())), preferred_element_type=F32)


def moe_kernel(ids_hbm, wgt_hbm, x_hbm, dout_hbm, win_hbm, wout_hbm,
               out_ref, gwin_ref, gwout_ref, gwg_ref, acc_ref, qlast_ref, rdx,
               ids_ref, wgt_ref, x_v, dout_v, win_v, wout_v, rank_v, p_v, q0_v, q1_v, dyflat_v, gate_v, cols_v,
               sx, rx, sdy, rdy, sy, ry, sdx, h_v, gp_v, da_v, xt_v, before_v, wg_part, wg_mate, wg_chip,
               load_sem, send_sem, recv_sem, wg_send, wg_recv):
    tok = x_v.shape[0]
    d_hid = win_v.shape[1]
    half = x_v.shape[1] // 2
    me = lax.axis_index('ep')
    core, col, row = me % 2, (me // 2) % 2, me // 4

    def peer(d):
        return 4 * ((row + d // 4) % 2) + 2 * ((col + (d // 2) % 2) % 2) + (core + d % 2) % 2

    def remote(phase, src, dst, d):
        return pltpu.make_async_remote_copy(
            src_ref=src.at[pl.ds(d * ROWS, ROWS)], dst_ref=dst.at[pl.ds(d * ROWS, ROWS)], send_sem=send_sem.at[phase, d], recv_sem=recv_sem.at[phase, d],
            device_id=(peer(d),), device_id_type=MESH)

    barrier = pltpu.get_barrier_semaphore()
    for d in range(1, N_DEV):
        pl.semaphore_signal(barrier, inc=1, device_id=(peer(d),), device_id_type=MESH)
    loads = [pltpu.make_async_copy(src, dst, load_sem.at[i]) for i, (src, dst) in enumerate(
        ((ids_hbm, ids_ref), (x_hbm, x_v), (wgt_hbm, wgt_ref), (dout_hbm, dout_v), (win_hbm, win_v), (wout_hbm, wout_v)))]
    for ld in loads:
        ld.start()

    rel = lax.broadcasted_iota(jnp.int32, (16, tok), 0) ^ me
    before_v[...] = jnp.where(lax.broadcasted_iota(jnp.int32, (tok, tok), 0) < lax.broadcasted_iota(jnp.int32, (tok, tok), 1), 1.0, 0.0).astype(BF16)
    slot = lax.broadcasted_iota(jnp.int32, (ROWS, tok), 0).astype(F32)
    loads[0].wait()
    ids0 = ids_ref[0:1, :]
    ids1 = ids_ref[1:2, :]
    hit0 = rel == ids0
    hit1 = rel == ids1
    hot = jnp.where(hit0 | hit1, 1.0, 0.0).astype(BF16)
    rank = dot_nn(hot, before_v[...])
    rank0 = jnp.where(hit0, rank, -1.0)
    rank1 = jnp.where(hit1, rank, -1.0)
    rank_v[0:16, :] = rank0
    rank_v[16:32, :] = rank1

    loads[1].wait()
    for d in (2, 4, 3, 5, 6, 7, 1, 0):
        pick0 = jnp.where(rank_v[d:d + 1, :] == slot, 1.0, 0.0)
        pick1 = jnp.where(rank_v[16 + d:17 + d, :] == slot, 1.0, 0.0)
        block = dot_nn((pick0 + pick1).astype(BF16), x_v[...]).astype(BF16)
        if d == 0:
            rx[0:ROWS] = block
        else:
            sx[d * ROWS:(d + 1) * ROWS] = block
            if d == 2:
                pl.semaphore_wait(barrier, N_DEV - 1)
            remote(0, sx, rx, d).start()
        p_v[d, :, 0:tok] = pick0.astype(BF16)
        p_v[d, :, tok:2 * tok] = pick1.astype(BF16)

    stack = jnp.concatenate([rank0, rank1, jnp.broadcast_to(ids0.astype(F32), (16, tok)),
                             jnp.broadcast_to(ids1.astype(F32), (16, tok)), jnp.zeros((64, tok), F32)], axis=0)
    cols_v[...] = stack.T
    loads[2].wait()
    logits = dot_nt(x_v[...], wgt_ref[...])
    lane8 = lax.broadcasted_iota(jnp.int32, (tok, N_DEV), 1).astype(F32)
    sel0 = jnp.sum(jnp.where(lane8 == cols_v[:, 32:33], logits, 0.0), axis=1, keepdims=True)
    sel1 = jnp.sum(jnp.where(lane8 == cols_v[:, 48:49], logits, 0.0), axis=1, keepdims=True)
    top = jnp.maximum(sel0, sel1)
    e0 = jnp.exp(sel0 - top)
    e1 = jnp.exp(sel1 - top)
    gate_v[0] = e0 / (e0 + e1)
    gate_v[1] = e1 / (e0 + e1)
    loads[3].wait()
    dout_f = dout_v[...].astype(F32)
    dyflat_v[0:tok, :] = (gate_v[0] * dout_f).astype(BF16)
    dyflat_v[tok:2 * tok, :] = (gate_v[1] * dout_f).astype(BF16)
    for d in (2, 4, 3, 5, 6, 7, 1, 0):
        block = dot_nn(p_v[d], dyflat_v[...]).astype(BF16)
        if d == 0:
            rdy[0:ROWS] = block
        else:
            sdy[d * ROWS:(d + 1) * ROWS] = block
            remote(1, sdy, rdy, d).start()

    hid = 512
    loads[4].wait()
    loads[5].wait()
    for c in range(4):
        for d in (2 * c, 2 * c + 1):
            if d:
                remote(0, sx, rx, d).wait_recv()
        rows = slice(2 * ROWS * c, 2 * ROWS * (c + 1))
        x_c = rx[rows]

        def fwd_tile(j, carry):
            cols = pl.ds(pl.multiple_of(j * hid, hid), hid)
            a = dot_nn(x_c, win_v[:, cols])
            sq = a * a
            t = jnp.tanh(SQRT_2_PI * (a + CUBIC * (a * sq)))
            cdf = 0.5 * (1.0 + t)
            h_v[rows, cols] = (a * cdf).astype(BF16)
            gp_v[rows, cols] = cdf + (0.5 * a) * (1.0 - t * t) * (SQRT_2_PI * (1.0 + (3.0 * CUBIC) * sq))
            return carry

        lax.fori_loop(0, d_hid // hid, fwd_tile, 0)
        y_c = dot_nn(h_v[rows, :], wout_v[...]).astype(BF16)
        for i, d in enumerate((2 * c, 2 * c + 1)):
            block = y_c[i * ROWS:(i + 1) * ROWS]
            if d == 0:
                ry[0:ROWS] = block
            else:
                sy[d * ROWS:(d + 1) * ROWS] = block
                remote(2, sy, ry, d).start()

    slot_l = lax.broadcasted_iota(jnp.int32, (tok, ROWS), 1).astype(F32)
    for d in range(N_DEV):
        q0_v[:, d * ROWS:(d + 1) * ROWS] = jnp.where(cols_v[:, d:d + 1] == slot_l, 1.0, 0.0).astype(BF16)
        q1_v[:, d * ROWS:(d + 1) * ROWS] = jnp.where(cols_v[:, 16 + d:17 + d] == slot_l, 1.0, 0.0).astype(BF16)

    def bwd_chunk(c):
        for d in (2 * c, 2 * c + 1):
            if d:
                remote(1, sdy, rdy, d).wait_recv()
        rows = slice(2 * ROWS * c, 2 * ROWS * (c + 1))
        dy_c = rdy[rows]

        def bwd_tile(j, carry):
            cols = pl.ds(pl.multiple_of(j * hid, hid), hid)
            dh = dot_nt(dy_c, wout_v[cols, :])
            da_v[rows, cols] = (dh * gp_v[rows, cols]).astype(BF16)
            return carry

        lax.fori_loop(0, d_hid // hid, bwd_tile, 0)
        dx_c = dot_nt(da_v[rows, :], win_v[...]).astype(BF16)
        for i, d in enumerate((2 * c, 2 * c + 1)):
            block = dx_c[i * ROWS:(i + 1) * ROWS]
            if d == 0:
                rdx[0:ROWS] = block
            else:
                sdx[d * ROWS:(d + 1) * ROWS] = block
                if c == 0:
                    remote(3, sdx, rdx, d).start()

    for c in range(4):
        bwd_chunk(c)
    for d in DX_EARLY:
        remote(3, sdx, rdx, d).start()

    xt_v[...] = rx[...].T
    wt = 256

    def grad_tile(j, carry):
        cols = pl.ds(pl.multiple_of(j * wt, wt), wt)
        gwout_ref[cols, :] = dot_tn(h_v[:, cols], rdy[...])
        gwin_ref[:, cols] = dot_nn(xt_v[...], da_v[:, cols])
        return carry

    lax.fori_loop(0, d_hid // wt, grad_tile, 0)

    for d in range(1, 6):
        remote(2, sy, ry, d).wait_recv()
    span = slice(0, 6 * ROWS)
    y0 = dot_nn(q0_v[:, span], ry[span])
    y1 = dot_nn(q1_v[:, span], ry[span])
    for d in (6, 7):
        remote(2, sy, ry, d).wait_recv()
    span = slice(6 * ROWS, 8 * ROWS)
    y0 = y0 + dot_nn(q0_v[:, span], ry[span])
    y1 = y1 + dot_nn(q1_v[:, span], ry[span])
    g0 = gate_v[0]
    g1 = gate_v[1]
    dout_f = dout_v[...].astype(F32)
    dg0 = jnp.sum(dout_f * y0, axis=1, keepdims=True)
    dg1 = jnp.sum(dout_f * y1, axis=1, keepdims=True)
    mean = g0 * dg0 + g1 * dg1
    d_log = (jnp.where(lane8 == cols_v[:, 32:33], g0 * (dg0 - mean), 0.0)
             + jnp.where(lane8 == cols_v[:, 48:49], g1 * (dg1 - mean), 0.0)).astype(BF16)
    for i in range(2):
        wg_part[i] = dot_tn(d_log, x_v[:, i * half:(i + 1) * half])

    def wg_copy(i, src, dst, d):
        return pltpu.make_async_remote_copy(
            src_ref=src, dst_ref=dst, send_sem=wg_send.at[i], recv_sem=wg_recv.at[i],
            device_id=(peer(d),), device_id_type=MESH)

    chip = 2 * row + col
    to_mate = wg_copy(0, wg_part.at[1 - core], wg_mate, 1)
    to_mate.start()
    out_ref[...] = (g0 * y0 + g1 * y1).astype(BF16)
    acc = dot_nn(d_log, wgt_ref[...])
    to_mate.wait_recv()
    wg_chip[chip] = wg_part[core] + wg_mate[...]
    to_chips = [wg_copy(1 + i, wg_chip.at[chip], wg_chip.at[chip], 2 * (i + 1)) for i in range(3)]
    for cp in to_chips:
        cp.start()
    for d in DX_LATE:
        remote(3, sdx, rdx, d).start()

    for c in (0, 3):
        for d in (2 * c, 2 * c + 1):
            if d:
                remote(3, sdx, rdx, d).wait_recv()
        span = slice(2 * ROWS * c, 2 * ROWS * (c + 1))
        acc = acc + dot_nn(q0_v[:, span] + q1_v[:, span], rdx[span])
    acc_ref[...] = acc
    span = slice(2 * ROWS, 6 * ROWS)
    qlast_ref[...] = q0_v[:, span] + q1_v[:, span]
    for cp in to_chips:
        cp.wait_recv()
    gwg_ref[core] = (wg_chip[0] + wg_chip[1]) + (wg_chip[2] + wg_chip[3])
    swap = wg_copy(4, gwg_ref.at[core], gwg_ref.at[core], 1)
    swap.start()
    to_mate.wait_send()
    for d in range(1, N_DEV):
        remote(0, sx, rx, d).wait_send()
        remote(1, sdy, rdy, d).wait_send()
        remote(2, sy, ry, d).wait_send()
    for cp in to_chips:
        cp.wait_send()
    swap.wait()
    for d in (2, 4, 3, 5):
        remote(3, sdx, rdx, d).wait_recv()
    for d in range(1, N_DEV):
        remote(3, sdx, rdx, d).wait_send()


def finish_kernel(out_v, gwin_v, gwout_v, gwg_v, acc_v, qlast_v, dx_v,
                  out_hbm, gx_hbm, gwin_hbm, gwout_hbm, gwg_hbm, gx_v, sem):
    half = gwg_v.shape[2]
    pieces = [(gwin_v, gwin_hbm), (gwout_v, gwout_hbm), (out_v, out_hbm), (gwg_v.at[0], gwg_hbm.at[:, pl.ds(0, half)]),
              (gwg_v.at[1], gwg_hbm.at[:, pl.ds(half, half)]), (gx_v, gx_hbm)]
    stores = [pltpu.make_async_copy(src, dst, sem.at[i]) for i, (src, dst) in enumerate(pieces)]
    for st in stores[:-1]:
        st.start()
    gx_v[...] = (acc_v[...] + dot_nn(qlast_v[...], dx_v[2 * ROWS:6 * ROWS])).astype(BF16)
    stores[-1].start()
    for st in stores:
        st.wait()


def local_block(tokens, grad_out, expert_ids, w_gate, w_in, w_out):
    tok, d_model = tokens.shape
    n_exp = w_gate.shape[1]
    d_hid = w_in.shape[2]
    slots = n_exp * ROWS
    vmem = pl.BlockSpec(memory_space=pltpu.VMEM)
    hbm = pl.BlockSpec(memory_space=pl.ANY)
    blocks = pltpu.VMEM((slots, d_model), BF16)
    args = [pltpu.with_memory_space_constraint(a, pltpu.HBM)
            for a in (expert_ids.T, w_gate.T, tokens, grad_out, w_in[0], w_out[0])]
    kept = pl.pallas_call(
        moe_kernel,
        out_shape=(pltpu.VMEM((tok, d_model), BF16), pltpu.VMEM((d_model, d_hid), F32), pltpu.VMEM((d_hid, d_model), F32),
                   pltpu.VMEM((2, n_exp, d_model // 2), F32), pltpu.VMEM((tok, d_model), F32),
                   pltpu.VMEM((tok, 4 * ROWS), BF16), pltpu.VMEM((slots, d_model), BF16)),
        in_specs=[hbm] * 6,
        out_specs=(vmem,) * 7,
        scratch_shapes=[
            pltpu.VMEM((2, tok), jnp.int32), pltpu.VMEM((n_exp, d_model), BF16),
            pltpu.VMEM((tok, d_model), BF16), pltpu.VMEM((tok, d_model), BF16),
            pltpu.VMEM((d_model, d_hid), BF16), pltpu.VMEM((d_hid, d_model), BF16),
            pltpu.VMEM((32, tok), F32), pltpu.VMEM((n_exp, ROWS, 2 * tok), BF16),
            pltpu.VMEM((tok, slots), BF16), pltpu.VMEM((tok, slots), BF16),
            pltpu.VMEM((2 * tok, d_model), BF16), pltpu.VMEM((2, tok, 1), F32), pltpu.VMEM((tok, 128), F32),
            blocks, blocks, blocks, blocks, blocks, blocks, blocks,
            pltpu.VMEM((slots, d_hid), BF16), pltpu.VMEM((slots, d_hid), F32), pltpu.VMEM((slots, d_hid), BF16),
            pltpu.VMEM((d_model, slots), BF16), pltpu.VMEM((tok, tok), BF16),
            pltpu.VMEM((2, n_exp, d_model // 2), F32), pltpu.VMEM((n_exp, d_model // 2), F32), pltpu.VMEM((4, n_exp, d_model // 2), F32),
            pltpu.SemaphoreType.DMA((6,)), pltpu.SemaphoreType.DMA((4, n_exp)), pltpu.SemaphoreType.DMA((4, n_exp)),
            pltpu.SemaphoreType.DMA((5,)), pltpu.SemaphoreType.DMA((5,)),
        ],
        compiler_params=pltpu.CompilerParams(collective_id=0, has_side_effects=True, vmem_limit_bytes=46 * 1024 * 1024),
        name='moe_step',
    )(*args)
    out, gx, gwin, gwout, gwg = pl.pallas_call(
        finish_kernel,
        out_shape=(jax.ShapeDtypeStruct((tok, d_model), BF16), jax.ShapeDtypeStruct((tok, d_model), BF16),
                   jax.ShapeDtypeStruct((d_model, d_hid), F32), jax.ShapeDtypeStruct((d_hid, d_model), F32),
                   jax.ShapeDtypeStruct((n_exp, d_model), F32)),
        in_specs=[vmem] * 7,
        out_specs=(hbm,) * 5,
        scratch_shapes=[pltpu.VMEM((tok, d_model), BF16), pltpu.SemaphoreType.DMA((6,))],
        compiler_params=pltpu.CompilerParams(vmem_limit_bytes=16 * 1024 * 1024),
        name='moe_finish',
    )(*kept)
    return out, gx, gwin[None], gwout[None], gwg.T


def solution(mesh):
    return jax.shard_map(local_block, mesh=mesh, in_specs=(P('ep'), P('ep'), P('ep'), P(), P('ep'), P('ep')), out_specs=(P('ep'), P('ep'), P('ep'), P('ep'), P()), check_vma=False)
```

```python
import functools

import jax
import jax.numpy as jnp
from jax import lax
from jax.experimental import pallas as pl
from jax.experimental.pallas import tpu as pltpu
from jax.sharding import PartitionSpec as P

N_DEV = 8
DX_EARLY = (1, 2, 4, 6, 3, 5)
DX_LATE = (7,)
ROWS = 128
MESH = pl.DeviceIdType.MESH
F32 = jnp.float32
BF16 = jnp.bfloat16
SQRT_2_PI = 0.7978845608028654
CUBIC = 0.044715


def dot_nn(a, b):
    return lax.dot_general(a, b, (((1,), (0,)), ((), ())), preferred_element_type=F32)


def dot_nt(a, b):
    return lax.dot_general(a, b, (((1,), (1,)), ((), ())), preferred_element_type=F32)


def dot_tn(a, b):
    return lax.dot_general(a, b, (((0,), (0,)), ((), ())), preferred_element_type=F32)


def moe_kernel(ids_hbm, wgt_hbm, x_hbm, dout_hbm, win_hbm, wout_hbm,
               out_ref, gwin_ref, gwout_ref, gwg_ref, acc_ref, q01_ref, rdx,
               ids_ref, wgt_ref, x_v, dout_v, win_v, wout_v, rank_v, p_v, q0_v, q1_v, dyflat_v, gate_v, cols_v,
               sx, rx, sdy, rdy, sy, ry, sdx, h_v, gp_v, da_v, xt_v, before_v, wg_part, wg_mate, wg_chip,
               load_sem, send_sem, recv_sem, wg_send, wg_recv):
    tok = x_v.shape[0]
    d_hid = win_v.shape[1]
    half = x_v.shape[1] // 2
    me = lax.axis_index('ep')
    core, col, row = me % 2, (me // 2) % 2, me // 4

    def peer(d):
        return 4 * ((row + d // 4) % 2) + 2 * ((col + (d // 2) % 2) % 2) + (core + d % 2) % 2

    def remote(phase, src, dst, d):
        return pltpu.make_async_remote_copy(
            src_ref=src.at[pl.ds(d * ROWS, ROWS)], dst_ref=dst.at[pl.ds(d * ROWS, ROWS)], send_sem=send_sem.at[phase, d], recv_sem=recv_sem.at[phase, d],
            device_id=(peer(d),), device_id_type=MESH)

    barrier = pltpu.get_barrier_semaphore()
    for d in range(1, N_DEV):
        pl.semaphore_signal(barrier, inc=1, device_id=(peer(d),), device_id_type=MESH)
    loads = [pltpu.make_async_copy(src, dst, load_sem.at[i]) for i, (src, dst) in enumerate(
        ((ids_hbm, ids_ref), (x_hbm, x_v), (wgt_hbm, wgt_ref), (dout_hbm, dout_v), (win_hbm, win_v), (wout_hbm, wout_v)))]
    for ld in loads:
        ld.start()

    rel = lax.broadcasted_iota(jnp.int32, (16, tok), 0) ^ me
    lane2 = lax.broadcasted_iota(jnp.int32, (ROWS, 2 * ROWS), 1)
    before_v[...] = jnp.where((lax.broadcasted_iota(jnp.int32, (ROWS, 2 * ROWS), 0) < lane2) | (lane2 >= ROWS), 1.0, 0.0).astype(BF16)
    slot = lax.broadcasted_iota(jnp.int32, (ROWS, tok), 0).astype(F32)
    loads[0].wait()
    ids0 = ids_ref[0:1, :]
    ids1 = ids_ref[1:2, :]
    hit0 = rel == ids0
    hit1 = rel == ids1
    hot = jnp.where(hit0 | hit1, 1.0, 0.0).astype(BF16)
    groups = [slice(g * ROWS, (g + 1) * ROWS) for g in range(tok // ROWS)]
    counts = dot_nn(jnp.concatenate([hot[:, g] for g in groups], axis=0), before_v[...])
    rank, base = [], 0.0
    for g in range(tok // ROWS):
        part = counts[16 * g:16 * (g + 1)]
        rank.append(part[:, 0:ROWS] + base)
        base = base + part[:, ROWS:2 * ROWS]
    rank = jnp.concatenate(rank, axis=1)
    rank0 = jnp.where(hit0, rank, -1.0)
    rank1 = jnp.where(hit1, rank, -1.0)
    rank_v[0:16, :] = rank0
    rank_v[16:32, :] = rank1

    loads[1].wait()
    for d in (2, 4, 3, 5, 6, 7, 1, 0):
        pick0 = jnp.where(rank_v[d:d + 1, :] == slot, 1.0, 0.0)
        pick1 = jnp.where(rank_v[16 + d:17 + d, :] == slot, 1.0, 0.0)
        block = dot_nn((pick0 + pick1).astype(BF16), x_v[...]).astype(BF16)
        if d == 0:
            rx[0:ROWS] = block
        else:
            sx[d * ROWS:(d + 1) * ROWS] = block
            if d == 2:
                pl.semaphore_wait(barrier, N_DEV - 1)
            remote(0, sx, rx, d).start()
        p_v[d, :, 0:tok] = pick0.astype(BF16)
        p_v[d, :, tok:2 * tok] = pick1.astype(BF16)

    stack = jnp.concatenate([rank0, rank1, jnp.broadcast_to(ids0.astype(F32), (16, tok)),
                             jnp.broadcast_to(ids1.astype(F32), (16, tok)), jnp.zeros((64, tok), F32)], axis=0)
    cols_v[...] = stack.T
    loads[2].wait()
    logits = dot_nt(x_v[...], wgt_ref[...])
    lane8 = lax.broadcasted_iota(jnp.int32, (tok, N_DEV), 1).astype(F32)
    sel0 = jnp.sum(jnp.where(lane8 == cols_v[:, 32:33], logits, 0.0), axis=1, keepdims=True)
    sel1 = jnp.sum(jnp.where(lane8 == cols_v[:, 48:49], logits, 0.0), axis=1, keepdims=True)
    top = jnp.maximum(sel0, sel1)
    e0 = jnp.exp(sel0 - top)
    e1 = jnp.exp(sel1 - top)
    gate_v[0] = e0 / (e0 + e1)
    gate_v[1] = e1 / (e0 + e1)
    loads[3].wait()
    dout_f = dout_v[...].astype(F32)
    dyflat_v[0:tok, :] = (gate_v[0] * dout_f).astype(BF16)
    dyflat_v[tok:2 * tok, :] = (gate_v[1] * dout_f).astype(BF16)
    for d in (2, 4, 3, 5, 6, 7, 1, 0):
        block = dot_nn(p_v[d], dyflat_v[...]).astype(BF16)
        if d == 0:
            rdy[0:ROWS] = block
        else:
            sdy[d * ROWS:(d + 1) * ROWS] = block
            remote(1, sdy, rdy, d).start()

    hid = 512
    loads[4].wait()
    loads[5].wait()
    def fwd_chunk(c, carry):
        @pl.when(c > 0)
        def _():
            remote(0, sx, rx, 2 * c).wait_recv()

        remote(0, sx, rx, 2 * c + 1).wait_recv()
        rows = pl.ds(pl.multiple_of(c * (2 * ROWS), 2 * ROWS), 2 * ROWS)
        x_c = rx[rows]

        def fwd_tile(j, inner):
            cols = pl.ds(pl.multiple_of(j * hid, hid), hid)
            a = dot_nn(x_c, win_v[:, cols])
            sq = a * a
            t = jnp.tanh(SQRT_2_PI * (a + CUBIC * (a * sq)))
            cdf = 0.5 * (1.0 + t)
            h_v[rows, cols] = (a * cdf).astype(BF16)
            gp_v[rows, cols] = cdf + (0.5 * a) * (1.0 - t * t) * (SQRT_2_PI * (1.0 + (3.0 * CUBIC) * sq))
            return inner

        lax.fori_loop(0, d_hid // hid, fwd_tile, 0)
        sy[rows] = dot_nn(h_v[rows], wout_v[...]).astype(BF16)

        @pl.when(c > 0)
        def _():
            remote(2, sy, ry, 2 * c).start()

        remote(2, sy, ry, 2 * c + 1).start()
        return carry

    lax.fori_loop(0, N_DEV // 2, fwd_chunk, 0)
    ry[0:ROWS] = sy[0:ROWS]

    slot_l = lax.broadcasted_iota(jnp.int32, (tok, ROWS), 1).astype(F32)
    for d in range(N_DEV):
        span = slice(d * ROWS, (d + 1) * ROWS)
        own0 = jnp.where(cols_v[:, d:d + 1] == slot_l, 1.0, 0.0)
        own1 = jnp.where(cols_v[:, 16 + d:17 + d] == slot_l, 1.0, 0.0)
        q0_v[:, span] = own0.astype(BF16)
        q1_v[:, span] = own1.astype(BF16)
        q01_ref[:, span] = (own0 + own1).astype(BF16)

    def bwd_chunk(c, carry):
        @pl.when(c > 0)
        def _():
            remote(1, sdy, rdy, 2 * c).wait_recv()

        remote(1, sdy, rdy, 2 * c + 1).wait_recv()
        rows = pl.ds(pl.multiple_of(c * (2 * ROWS), 2 * ROWS), 2 * ROWS)
        dy_c = rdy[rows]

        def bwd_tile(j, inner):
            cols = pl.ds(pl.multiple_of(j * hid, hid), hid)
            dh = dot_nt(dy_c, wout_v[cols, :])
            da_v[rows, cols] = (dh * gp_v[rows, cols]).astype(BF16)
            return inner

        lax.fori_loop(0, d_hid // hid, bwd_tile, 0)
        sdx[rows] = dot_nt(da_v[rows], win_v[...]).astype(BF16)
        return carry

    lax.fori_loop(0, N_DEV // 2, bwd_chunk, 0)
    rdx[0:ROWS] = sdx[0:ROWS]
    for d in DX_EARLY:
        remote(3, sdx, rdx, d).start()

    xt_v[...] = rx[...].T
    wt = 256

    def grad_tile(j, carry):
        cols = pl.ds(pl.multiple_of(j * wt, wt), wt)
        gwout_ref[cols, :] = dot_tn(h_v[:, cols], rdy[...])
        gwin_ref[:, cols] = dot_nn(xt_v[...], da_v[:, cols])
        return carry

    lax.fori_loop(0, d_hid // wt, grad_tile, 0)

    for d in range(1, 6):
        remote(2, sy, ry, d).wait_recv()
    span = slice(0, 6 * ROWS)
    y0 = dot_nn(q0_v[:, span], ry[span])
    y1 = dot_nn(q1_v[:, span], ry[span])
    for d in (6, 7):
        remote(2, sy, ry, d).wait_recv()
    span = slice(6 * ROWS, 8 * ROWS)
    y0 = y0 + dot_nn(q0_v[:, span], ry[span])
    y1 = y1 + dot_nn(q1_v[:, span], ry[span])
    g0 = gate_v[0]
    g1 = gate_v[1]
    dout_f = dout_v[...].astype(F32)
    dg0 = jnp.sum(dout_f * y0, axis=1, keepdims=True)
    dg1 = jnp.sum(dout_f * y1, axis=1, keepdims=True)
    mean = g0 * dg0 + g1 * dg1
    d_log = (jnp.where(lane8 == cols_v[:, 32:33], g0 * (dg0 - mean), 0.0)
             + jnp.where(lane8 == cols_v[:, 48:49], g1 * (dg1 - mean), 0.0)).astype(BF16)
    for i in range(2):
        wg_part[i] = dot_tn(d_log, x_v[:, i * half:(i + 1) * half])

    def wg_copy(i, src, dst, d):
        return pltpu.make_async_remote_copy(
            src_ref=src, dst_ref=dst, send_sem=wg_send.at[i], recv_sem=wg_recv.at[i],
            device_id=(peer(d),), device_id_type=MESH)

    chip = 2 * row + col
    to_mate = wg_copy(0, wg_part.at[1 - core], wg_mate, 1)
    to_mate.start()
    out_ref[...] = (g0 * y0 + g1 * y1).astype(BF16)
    acc_ref[...] = dot_nn(d_log, wgt_ref[...])
    to_mate.wait_recv()
    wg_chip[chip] = wg_part[core] + wg_mate[...]
    to_chips = [wg_copy(1 + i, wg_chip.at[chip], wg_chip.at[chip], 2 * (i + 1)) for i in range(3)]
    for cp in to_chips:
        cp.start()
    for d in DX_LATE:
        remote(3, sdx, rdx, d).start()

    for cp in to_chips:
        cp.wait_recv()
    gwg_ref[core] = (wg_chip[0] + wg_chip[1]) + (wg_chip[2] + wg_chip[3])
    swap = wg_copy(4, gwg_ref.at[core], gwg_ref.at[core], 1)
    swap.start()
    to_mate.wait_send()
    for d in range(1, N_DEV):
        remote(0, sx, rx, d).wait_send()
        remote(1, sdy, rdy, d).wait_send()
        remote(2, sy, ry, d).wait_send()
    for cp in to_chips:
        cp.wait_send()
    swap.wait()
    for d in range(1, N_DEV):
        remote(3, sdx, rdx, d).wait()


def finish_kernel(out_v, gwin_v, gwout_v, gwg_v, acc_v, q01_v, dx_v,
                  out_hbm, gx_hbm, gwin_hbm, gwout_hbm, gwg_hbm, gx_v, sem):
    half = gwg_v.shape[2]
    pieces = [(gwin_v, gwin_hbm), (gwout_v, gwout_hbm), (out_v, out_hbm), (gwg_v.at[0], gwg_hbm.at[:, pl.ds(0, half)]),
              (gwg_v.at[1], gwg_hbm.at[:, pl.ds(half, half)]), (gx_v, gx_hbm)]
    stores = [pltpu.make_async_copy(src, dst, sem.at[i]) for i, (src, dst) in enumerate(pieces)]
    for st in stores[:-1]:
        st.start()
    gx_v[...] = (acc_v[...] + dot_nn(q01_v[...], dx_v[...])).astype(BF16)
    stores[-1].start()
    for st in stores:
        st.wait()


def local_block(tokens, grad_out, expert_ids, w_gate, w_in, w_out):
    tok, d_model = tokens.shape
    n_exp = w_gate.shape[1]
    d_hid = w_in.shape[2]
    slots = n_exp * ROWS
    vmem = pl.BlockSpec(memory_space=pltpu.VMEM)
    hbm = pl.BlockSpec(memory_space=pl.ANY)
    blocks = pltpu.VMEM((slots, d_model), BF16)
    args = [pltpu.with_memory_space_constraint(a, pltpu.HBM)
            for a in (expert_ids.T, w_gate.T, tokens, grad_out, w_in[0], w_out[0])]
    kept = pl.pallas_call(
        moe_kernel,
        out_shape=(pltpu.VMEM((tok, d_model), BF16), pltpu.VMEM((d_model, d_hid), F32), pltpu.VMEM((d_hid, d_model), F32),
                   pltpu.VMEM((2, n_exp, d_model // 2), F32), pltpu.VMEM((tok, d_model), F32),
                   pltpu.VMEM((tok, slots), BF16), pltpu.VMEM((slots, d_model), BF16)),
        in_specs=[hbm] * 6,
        out_specs=(vmem,) * 7,
        scratch_shapes=[
            pltpu.VMEM((2, tok), jnp.int32), pltpu.VMEM((n_exp, d_model), BF16),
            pltpu.VMEM((tok, d_model), BF16), pltpu.VMEM((tok, d_model), BF16),
            pltpu.VMEM((d_model, d_hid), BF16), pltpu.VMEM((d_hid, d_model), BF16),
            pltpu.VMEM((32, tok), F32), pltpu.VMEM((n_exp, ROWS, 2 * tok), BF16),
            pltpu.VMEM((tok, slots), BF16), pltpu.VMEM((tok, slots), BF16),
            pltpu.VMEM((2 * tok, d_model), BF16), pltpu.VMEM((2, tok, 1), F32), pltpu.VMEM((tok, 128), F32),
            blocks, blocks, blocks, blocks, blocks, blocks, blocks,
            pltpu.VMEM((slots, d_hid), BF16), pltpu.VMEM((slots, d_hid), F32), pltpu.VMEM((slots, d_hid), BF16),
            pltpu.VMEM((d_model, slots), BF16), pltpu.VMEM((ROWS, 2 * ROWS), BF16),
            pltpu.VMEM((2, n_exp, d_model // 2), F32), pltpu.VMEM((n_exp, d_model // 2), F32), pltpu.VMEM((4, n_exp, d_model // 2), F32),
            pltpu.SemaphoreType.DMA((6,)), pltpu.SemaphoreType.DMA((4, n_exp)), pltpu.SemaphoreType.DMA((4, n_exp)),
            pltpu.SemaphoreType.DMA((5,)), pltpu.SemaphoreType.DMA((5,)),
        ],
        compiler_params=pltpu.CompilerParams(collective_id=0, has_side_effects=True, vmem_limit_bytes=46 * 1024 * 1024),
        name='moe_step',
    )(*args)
    out, gx, gwin, gwout, gwg = pl.pallas_call(
        finish_kernel,
        out_shape=(jax.ShapeDtypeStruct((tok, d_model), BF16), jax.ShapeDtypeStruct((tok, d_model), BF16),
                   jax.ShapeDtypeStruct((d_model, d_hid), F32), jax.ShapeDtypeStruct((d_hid, d_model), F32),
                   jax.ShapeDtypeStruct((n_exp, d_model), F32)),
        in_specs=[vmem] * 7,
        out_specs=(hbm,) * 5,
        scratch_shapes=[pltpu.VMEM((tok, d_model), BF16), pltpu.SemaphoreType.DMA((6,))],
        compiler_params=pltpu.CompilerParams(vmem_limit_bytes=16 * 1024 * 1024),
        name='moe_finish',
    )(*kept)
    return out, gx, gwin[None], gwout[None], gwg.T


def solution(mesh):
    return jax.shard_map(local_block, mesh=mesh, in_specs=(P('ep'), P('ep'), P('ep'), P(), P('ep'), P('ep')), out_specs=(P('ep'), P('ep'), P('ep'), P('ep'), P()), check_vma=False)
```

```python
import functools

import jax
import jax.numpy as jnp
from jax import lax
from jax.experimental import pallas as pl
from jax.experimental.pallas import tpu as pltpu
from jax.sharding import PartitionSpec as P

N_DEV = 8
DX_EARLY = (1, 2, 4, 6, 3)
DX_LATE = (7, 5)
ROWS = 128
MESH = pl.DeviceIdType.MESH
F32 = jnp.float32
BF16 = jnp.bfloat16
SQRT_2_PI = 0.7978845608028654
CUBIC = 0.044715


def dot_nn(a, b):
    return lax.dot_general(a, b, (((1,), (0,)), ((), ())), preferred_element_type=F32)


def dot_nt(a, b):
    return lax.dot_general(a, b, (((1,), (1,)), ((), ())), preferred_element_type=F32)


def dot_tn(a, b):
    return lax.dot_general(a, b, (((0,), (0,)), ((), ())), preferred_element_type=F32)


def moe_kernel(ids_hbm, wgt_hbm, x_hbm, dout_hbm, win_hbm, wout_hbm,
               out_ref, gwin_ref, gwout_ref, gwg_ref, acc_ref, q01_ref, rdx,
               ids_ref, wgt_ref, x_v, dout_v, win_v, wout_v, rank_v, q0_v, q1_v, dyflat_v, gate_v, cols_v,
               sx, rx, sdy, rdy, sy, ry, sdx, h_v, gp_v, da_v, xt_v, before_v, wg_part, wg_mate, wg_chip,
               load_sem, send_sem, recv_sem, wg_send, wg_recv):
    tok = x_v.shape[0]
    d_hid = win_v.shape[1]
    half = x_v.shape[1] // 2
    me = lax.axis_index('ep')
    core, col, row = me % 2, (me // 2) % 2, me // 4

    def peer(d):
        return 4 * ((row + d // 4) % 2) + 2 * ((col + (d // 2) % 2) % 2) + (core + d % 2) % 2

    def remote(phase, src, dst, d):
        return pltpu.make_async_remote_copy(
            src_ref=src.at[pl.ds(d * ROWS, ROWS)], dst_ref=dst.at[pl.ds(d * ROWS, ROWS)], send_sem=send_sem.at[phase, d], recv_sem=recv_sem.at[phase, d],
            device_id=(peer(d),), device_id_type=MESH)

    barrier = pltpu.get_barrier_semaphore()
    for d in range(1, N_DEV):
        pl.semaphore_signal(barrier, inc=1, device_id=(peer(d),), device_id_type=MESH)
    loads = [pltpu.make_async_copy(src, dst, load_sem.at[i]) for i, (src, dst) in enumerate(
        ((ids_hbm, ids_ref), (x_hbm, x_v), (wgt_hbm, wgt_ref), (dout_hbm, dout_v), (win_hbm, win_v), (wout_hbm, wout_v)))]
    for ld in loads:
        ld.start()

    rel = lax.broadcasted_iota(jnp.int32, (16, tok), 0) ^ me
    lane2 = lax.broadcasted_iota(jnp.int32, (ROWS, 2 * ROWS), 1)
    before_v[...] = jnp.where((lax.broadcasted_iota(jnp.int32, (ROWS, 2 * ROWS), 0) < lane2) | (lane2 >= ROWS), 1.0, 0.0).astype(BF16)
    slot = lax.broadcasted_iota(jnp.int32, (ROWS, tok), 0).astype(F32)
    loads[0].wait()
    ids0 = ids_ref[0:1, :]
    ids1 = ids_ref[1:2, :]
    hit0 = rel == ids0
    hit1 = rel == ids1
    hot = jnp.where(hit0 | hit1, 1.0, 0.0).astype(BF16)
    groups = [slice(g * ROWS, (g + 1) * ROWS) for g in range(tok // ROWS)]
    counts = dot_nn(jnp.concatenate([hot[:, g] for g in groups], axis=0), before_v[...])
    rank, base = [], 0.0
    for g in range(tok // ROWS):
        part = counts[16 * g:16 * (g + 1)]
        rank.append(part[:, 0:ROWS] + base)
        base = base + part[:, ROWS:2 * ROWS]
    rank = jnp.concatenate(rank, axis=1)
    rank0 = jnp.where(hit0, rank, -1.0)
    rank1 = jnp.where(hit1, rank, -1.0)
    rank_v[32:48, :] = jnp.where(hit0 | hit1, rank, -1.0)
    rank_v[0:16, :] = rank0
    rank_v[16:32, :] = rank1

    loads[1].wait()
    for d in (2, 4, 6, 3, 5, 7, 1, 0):
        pick = jnp.where(rank_v[32 + d:33 + d, :] == slot, 1.0, 0.0).astype(BF16)
        block = dot_nn(pick, x_v[...]).astype(BF16)
        if d == 0:
            rx[0:ROWS] = block
        else:
            sx[d * ROWS:(d + 1) * ROWS] = block
            if d == 2:
                pl.semaphore_wait(barrier, N_DEV - 1)
            remote(0, sx, rx, d).start()

    stack = jnp.concatenate([rank0, rank1, jnp.broadcast_to(ids0.astype(F32), (16, tok)),
                             jnp.broadcast_to(ids1.astype(F32), (16, tok)), jnp.zeros((64, tok), F32)], axis=0)
    cols_v[...] = stack.T
    loads[2].wait()
    logits = dot_nt(x_v[...], wgt_ref[...])
    lane8 = lax.broadcasted_iota(jnp.int32, (tok, N_DEV), 1).astype(F32)
    sel0 = jnp.sum(jnp.where(lane8 == cols_v[:, 32:33], logits, 0.0), axis=1, keepdims=True)
    sel1 = jnp.sum(jnp.where(lane8 == cols_v[:, 48:49], logits, 0.0), axis=1, keepdims=True)
    top = jnp.maximum(sel0, sel1)
    e0 = jnp.exp(sel0 - top)
    e1 = jnp.exp(sel1 - top)
    gate_v[0] = e0 / (e0 + e1)
    gate_v[1] = e1 / (e0 + e1)
    loads[3].wait()
    dout_f = dout_v[...].astype(F32)
    dyflat_v[0:tok, :] = (gate_v[0] * dout_f).astype(BF16)
    dyflat_v[tok:2 * tok, :] = (gate_v[1] * dout_f).astype(BF16)
    for d in (2, 4, 3, 5, 6, 7, 1, 0):
        pick0 = jnp.where(rank_v[d:d + 1, :] == slot, 1.0, 0.0).astype(BF16)
        pick1 = jnp.where(rank_v[16 + d:17 + d, :] == slot, 1.0, 0.0).astype(BF16)
        block = (dot_nn(pick0, dyflat_v[0:tok]) + dot_nn(pick1, dyflat_v[tok:2 * tok])).astype(BF16)
        if d == 0:
            rdy[0:ROWS] = block
        else:
            sdy[d * ROWS:(d + 1) * ROWS] = block
            remote(1, sdy, rdy, d).start()

    hid = 512
    loads[4].wait()
    loads[5].wait()
    def fwd_chunk(c, carry):
        @pl.when(c > 0)
        def _():
            remote(0, sx, rx, 2 * c).wait_recv()

        remote(0, sx, rx, 2 * c + 1).wait_recv()
        rows = pl.ds(pl.multiple_of(c * (2 * ROWS), 2 * ROWS), 2 * ROWS)
        x_c = rx[rows]

        def fwd_tile(j, inner):
            cols = pl.ds(pl.multiple_of(j * hid, hid), hid)
            a = dot_nn(x_c, win_v[:, cols])
            sq = a * a
            t = jnp.tanh(SQRT_2_PI * (a + CUBIC * (a * sq)))
            cdf = 0.5 * (1.0 + t)
            h_v[rows, cols] = (a * cdf).astype(BF16)
            gp_v[rows, cols] = cdf + (0.5 * a) * (1.0 - t * t) * (SQRT_2_PI * (1.0 + (3.0 * CUBIC) * sq))
            return inner

        lax.fori_loop(0, d_hid // hid, fwd_tile, 0)
        sy[rows] = dot_nn(h_v[rows], wout_v[...]).astype(BF16)

        @pl.when(c > 0)
        def _():
            remote(2, sy, ry, 2 * c).start()

        remote(2, sy, ry, 2 * c + 1).start()
        return carry

    lax.fori_loop(0, N_DEV // 2, fwd_chunk, 0)
    ry[0:ROWS] = sy[0:ROWS]

    slot_l = lax.broadcasted_iota(jnp.int32, (tok, ROWS), 1).astype(F32)
    for d in range(N_DEV):
        span = slice(d * ROWS, (d + 1) * ROWS)
        own0 = jnp.where(cols_v[:, d:d + 1] == slot_l, 1.0, 0.0)
        own1 = jnp.where(cols_v[:, 16 + d:17 + d] == slot_l, 1.0, 0.0)
        q0_v[:, span] = own0.astype(BF16)
        q1_v[:, span] = own1.astype(BF16)
        q01_ref[:, span] = (own0 + own1).astype(BF16)

    def bwd_chunk(c, carry):
        @pl.when(c > 0)
        def _():
            remote(1, sdy, rdy, 2 * c).wait_recv()

        remote(1, sdy, rdy, 2 * c + 1).wait_recv()
        rows = pl.ds(pl.multiple_of(c * (2 * ROWS), 2 * ROWS), 2 * ROWS)
        dy_c = rdy[rows]

        def bwd_tile(j, inner):
            cols = pl.ds(pl.multiple_of(j * hid, hid), hid)
            dh = dot_nt(dy_c, wout_v[cols, :])
            da_v[rows, cols] = (dh * gp_v[rows, cols]).astype(BF16)
            return inner

        lax.fori_loop(0, d_hid // hid, bwd_tile, 0)
        sdx[rows] = dot_nt(da_v[rows], win_v[...]).astype(BF16)
        return carry

    lax.fori_loop(0, N_DEV // 2, bwd_chunk, 0)
    rdx[0:ROWS] = sdx[0:ROWS]
    for d in DX_EARLY:
        remote(3, sdx, rdx, d).start()

    xt_v[...] = rx[...].T
    wt = 256

    def grad_tile(j, carry):
        cols = pl.ds(pl.multiple_of(j * wt, wt), wt)
        gwout_ref[cols, :] = dot_tn(h_v[:, cols], rdy[...])
        gwin_ref[:, cols] = dot_nn(xt_v[...], da_v[:, cols])
        return carry

    lax.fori_loop(0, d_hid // wt, grad_tile, 0)

    for d in range(1, 6):
        remote(2, sy, ry, d).wait_recv()
    span = slice(0, 6 * ROWS)
    y0 = dot_nn(q0_v[:, span], ry[span])
    y1 = dot_nn(q1_v[:, span], ry[span])
    for d in (6, 7):
        remote(2, sy, ry, d).wait_recv()
    span = slice(6 * ROWS, 8 * ROWS)
    y0 = y0 + dot_nn(q0_v[:, span], ry[span])
    y1 = y1 + dot_nn(q1_v[:, span], ry[span])
    g0 = gate_v[0]
    g1 = gate_v[1]
    dout_f = dout_v[...].astype(F32)
    dg0 = jnp.sum(dout_f * y0, axis=1, keepdims=True)
    dg1 = jnp.sum(dout_f * y1, axis=1, keepdims=True)
    mean = g0 * dg0 + g1 * dg1
    d_log = (jnp.where(lane8 == cols_v[:, 32:33], g0 * (dg0 - mean), 0.0)
             + jnp.where(lane8 == cols_v[:, 48:49], g1 * (dg1 - mean), 0.0)).astype(BF16)
    for i in range(2):
        wg_part[i] = dot_tn(d_log, x_v[:, i * half:(i + 1) * half])

    def wg_copy(i, src, dst, d):
        return pltpu.make_async_remote_copy(
            src_ref=src, dst_ref=dst, send_sem=wg_send.at[i], recv_sem=wg_recv.at[i],
            device_id=(peer(d),), device_id_type=MESH)

    chip = 2 * row + col
    to_mate = wg_copy(0, wg_part.at[1 - core], wg_mate, 1)
    to_mate.start()
    out_ref[...] = (g0 * y0 + g1 * y1).astype(BF16)
    acc_ref[...] = dot_nn(d_log, wgt_ref[...])
    to_mate.wait_recv()
    wg_chip[chip] = wg_part[core] + wg_mate[...]
    to_chips = [wg_copy(1 + i, wg_chip.at[chip], wg_chip.at[chip], 2 * (i + 1)) for i in range(3)]
    for cp in to_chips:
        cp.start()
    for d in DX_LATE:
        remote(3, sdx, rdx, d).start()

    for cp in to_chips:
        cp.wait_recv()
    gwg_ref[core] = (wg_chip[0] + wg_chip[1]) + (wg_chip[2] + wg_chip[3])
    swap = wg_copy(4, gwg_ref.at[core], gwg_ref.at[core], 1)
    swap.start()
    to_mate.wait_send()
    for d in range(1, N_DEV):
        remote(0, sx, rx, d).wait_send()
        remote(1, sdy, rdy, d).wait_send()
        remote(2, sy, ry, d).wait_send()
    for cp in to_chips:
        cp.wait_send()
    swap.wait()
    for d in range(1, N_DEV):
        remote(3, sdx, rdx, d).wait()


def finish_kernel(out_v, gwin_v, gwout_v, gwg_v, acc_v, q01_v, dx_v,
                  out_hbm, gx_hbm, gwin_hbm, gwout_hbm, gwg_hbm, gx_v, sem):
    half = gwg_v.shape[2]
    pieces = [(gwin_v, gwin_hbm), (gwout_v, gwout_hbm), (out_v, out_hbm), (gwg_v.at[0], gwg_hbm.at[:, pl.ds(0, half)]),
              (gwg_v.at[1], gwg_hbm.at[:, pl.ds(half, half)]), (gx_v, gx_hbm)]
    stores = [pltpu.make_async_copy(src, dst, sem.at[i]) for i, (src, dst) in enumerate(pieces)]
    for st in stores[:-1]:
        st.start()
    gx_v[...] = (acc_v[...] + dot_nn(q01_v[...], dx_v[...])).astype(BF16)
    stores[-1].start()
    for st in stores:
        st.wait()


def local_block(tokens, grad_out, expert_ids, w_gate, w_in, w_out):
    tok, d_model = tokens.shape
    n_exp = w_gate.shape[1]
    d_hid = w_in.shape[2]
    slots = n_exp * ROWS
    vmem = pl.BlockSpec(memory_space=pltpu.VMEM)
    hbm = pl.BlockSpec(memory_space=pl.ANY)
    blocks = pltpu.VMEM((slots, d_model), BF16)
    args = [pltpu.with_memory_space_constraint(a, pltpu.HBM)
            for a in (expert_ids.T, w_gate.T, tokens, grad_out, w_in[0], w_out[0])]
    kept = pl.pallas_call(
        moe_kernel,
        out_shape=(pltpu.VMEM((tok, d_model), BF16), pltpu.VMEM((d_model, d_hid), F32), pltpu.VMEM((d_hid, d_model), F32),
                   pltpu.VMEM((2, n_exp, d_model // 2), F32), pltpu.VMEM((tok, d_model), F32),
                   pltpu.VMEM((tok, slots), BF16), pltpu.VMEM((slots, d_model), BF16)),
        in_specs=[hbm] * 6,
        out_specs=(vmem,) * 7,
        scratch_shapes=[
            pltpu.VMEM((2, tok), jnp.int32), pltpu.VMEM((n_exp, d_model), BF16),
            pltpu.VMEM((tok, d_model), BF16), pltpu.VMEM((tok, d_model), BF16),
            pltpu.VMEM((d_model, d_hid), BF16), pltpu.VMEM((d_hid, d_model), BF16),
            pltpu.VMEM((48, tok), F32),
            pltpu.VMEM((tok, slots), BF16), pltpu.VMEM((tok, slots), BF16),
            pltpu.VMEM((2 * tok, d_model), BF16), pltpu.VMEM((2, tok, 1), F32), pltpu.VMEM((tok, 128), F32),
            blocks, blocks, blocks, blocks, blocks, blocks, blocks,
            pltpu.VMEM((slots, d_hid), BF16), pltpu.VMEM((slots, d_hid), F32), pltpu.VMEM((slots, d_hid), BF16),
            pltpu.VMEM((d_model, slots), BF16), pltpu.VMEM((ROWS, 2 * ROWS), BF16),
            pltpu.VMEM((2, n_exp, d_model // 2), F32), pltpu.VMEM((n_exp, d_model // 2), F32), pltpu.VMEM((4, n_exp, d_model // 2), F32),
            pltpu.SemaphoreType.DMA((6,)), pltpu.SemaphoreType.DMA((4, n_exp)), pltpu.SemaphoreType.DMA((4, n_exp)),
            pltpu.SemaphoreType.DMA((5,)), pltpu.SemaphoreType.DMA((5,)),
        ],
        compiler_params=pltpu.CompilerParams(collective_id=0, has_side_effects=True, vmem_limit_bytes=46 * 1024 * 1024),
        name='moe_step',
    )(*args)
    out, gx, gwin, gwout, gwg = pl.pallas_call(
        finish_kernel,
        out_shape=(jax.ShapeDtypeStruct((tok, d_model), BF16), jax.ShapeDtypeStruct((tok, d_model), BF16),
                   jax.ShapeDtypeStruct((d_model, d_hid), F32), jax.ShapeDtypeStruct((d_hid, d_model), F32),
                   jax.ShapeDtypeStruct((n_exp, d_model), F32)),
        in_specs=[vmem] * 7,
        out_specs=(hbm,) * 5,
        scratch_shapes=[pltpu.VMEM((tok, d_model), BF16), pltpu.SemaphoreType.DMA((6,))],
        compiler_params=pltpu.CompilerParams(vmem_limit_bytes=16 * 1024 * 1024),
        name='moe_finish',
    )(*kept)
    return out, gx, gwin[None], gwout[None], gwg.T


def solution(mesh):
    return jax.shard_map(local_block, mesh=mesh, in_specs=(P('ep'), P('ep'), P('ep'), P(), P('ep'), P('ep')), out_specs=(P('ep'), P('ep'), P('ep'), P('ep'), P()), check_vma=False)
```

```python
import functools

import jax
import jax.numpy as jnp
from jax import lax
from jax.experimental import pallas as pl
from jax.experimental.pallas import tpu as pltpu
from jax.sharding import PartitionSpec as P

N_DEV = 8
DX_EARLY = (1, 2, 4, 6, 3)
DX_LATE = (7, 5)
ROWS = 128
MESH = pl.DeviceIdType.MESH
F32 = jnp.float32
BF16 = jnp.bfloat16
SQRT_2_PI = 0.7978845608028654
CUBIC = 0.044715


def dot_nn(a, b):
    return lax.dot_general(a, b, (((1,), (0,)), ((), ())), preferred_element_type=F32)


def dot_nt(a, b):
    return lax.dot_general(a, b, (((1,), (1,)), ((), ())), preferred_element_type=F32)


def dot_tn(a, b):
    return lax.dot_general(a, b, (((0,), (0,)), ((), ())), preferred_element_type=F32)


def moe_kernel(ids_hbm, wgt_hbm, x_hbm, dout_hbm, win_hbm, wout_hbm,
               out_ref, gwin_ref, gwout_ref, gwg_ref, acc_ref, q01_ref, rdx,
               ids_ref, wgt_ref, x_v, dout_v, win_v, wout_v, rank_v, q0_v, q1_v, dyflat_v, gate_v, cols_v,
               sx, rx, sdy, rdy, sy, ry, sdx, h_v, gp_v, da_v, xt_v, before_v, wg_part, wg_mate, wg_chip,
               load_sem, send_sem, recv_sem, wg_send, wg_recv):
    tok = x_v.shape[0]
    d_hid = win_v.shape[1]
    half = x_v.shape[1] // 2
    me = lax.axis_index('ep')
    core, col, row = me % 2, (me // 2) % 2, me // 4

    def peer(d):
        return 4 * ((row + d // 4) % 2) + 2 * ((col + (d // 2) % 2) % 2) + (core + d % 2) % 2

    def remote(phase, src, dst, d):
        return pltpu.make_async_remote_copy(
            src_ref=src.at[pl.ds(d * ROWS, ROWS)], dst_ref=dst.at[pl.ds(d * ROWS, ROWS)], send_sem=send_sem.at[phase, d], recv_sem=recv_sem.at[phase, d],
            device_id=(peer(d),), device_id_type=MESH)

    barrier = pltpu.get_barrier_semaphore()
    for d in range(1, N_DEV):
        pl.semaphore_signal(barrier, inc=1, device_id=(peer(d),), device_id_type=MESH)
    loads = [pltpu.make_async_copy(src, dst, load_sem.at[i]) for i, (src, dst) in enumerate(
        ((ids_hbm, ids_ref), (x_hbm, x_v), (wgt_hbm, wgt_ref), (dout_hbm, dout_v), (win_hbm, win_v), (wout_hbm, wout_v)))]
    for ld in loads:
        ld.start()

    rel = lax.broadcasted_iota(jnp.int32, (16, tok), 0) ^ me
    lane2 = lax.broadcasted_iota(jnp.int32, (ROWS, 2 * ROWS), 1)
    before_v[...] = jnp.where((lax.broadcasted_iota(jnp.int32, (ROWS, 2 * ROWS), 0) < lane2) | (lane2 >= ROWS), 1.0, 0.0).astype(BF16)
    slot = lax.broadcasted_iota(jnp.int32, (ROWS, tok), 0).astype(F32)
    loads[0].wait()
    ids0 = ids_ref[0:1, :]
    ids1 = ids_ref[1:2, :]
    hit0 = rel == ids0
    hit1 = rel == ids1
    hot = jnp.where(hit0 | hit1, 1.0, 0.0).astype(BF16)
    groups = [slice(g * ROWS, (g + 1) * ROWS) for g in range(tok // ROWS)]
    counts = dot_nn(jnp.concatenate([hot[:, g] for g in groups], axis=0), before_v[...])
    rank, base = [], 0.0
    for g in range(tok // ROWS):
        part = counts[16 * g:16 * (g + 1)]
        rank.append(part[:, 0:ROWS] + base)
        base = base + part[:, ROWS:2 * ROWS]
    rank = jnp.concatenate(rank, axis=1)
    rank0 = jnp.where(hit0, rank, -1.0)
    rank1 = jnp.where(hit1, rank, -1.0)
    rank_v[32:48, :] = jnp.where(hit0 | hit1, rank, -1.0)
    rank_v[0:16, :] = rank0
    rank_v[16:32, :] = rank1

    loads[1].wait()
    for group in ((2,), (4, 6), (3, 5), (7, 1), (0,)):
        pick = jnp.concatenate([jnp.where(rank_v[32 + d:33 + d, :] == slot, 1.0, 0.0).astype(BF16) for d in group], axis=0)
        blocks = dot_nn(pick, x_v[...]).astype(BF16)
        for i, d in enumerate(group):
            block = blocks[i * ROWS:(i + 1) * ROWS]
            if d == 0:
                rx[0:ROWS] = block
            else:
                sx[d * ROWS:(d + 1) * ROWS] = block
                if d == 2:
                    pl.semaphore_wait(barrier, N_DEV - 1)
                remote(0, sx, rx, d).start()

    stack = jnp.concatenate([rank0, rank1, jnp.broadcast_to(ids0.astype(F32), (16, tok)),
                             jnp.broadcast_to(ids1.astype(F32), (16, tok)), jnp.zeros((64, tok), F32)], axis=0)
    cols_v[...] = stack.T
    loads[2].wait()
    logits = dot_nt(x_v[...], wgt_ref[...])
    lane8 = lax.broadcasted_iota(jnp.int32, (tok, N_DEV), 1).astype(F32)
    sel0 = jnp.sum(jnp.where(lane8 == cols_v[:, 32:33], logits, 0.0), axis=1, keepdims=True)
    sel1 = jnp.sum(jnp.where(lane8 == cols_v[:, 48:49], logits, 0.0), axis=1, keepdims=True)
    top = jnp.maximum(sel0, sel1)
    e0 = jnp.exp(sel0 - top)
    e1 = jnp.exp(sel1 - top)
    gate_v[0] = e0 / (e0 + e1)
    gate_v[1] = e1 / (e0 + e1)
    loads[3].wait()
    dout_f = dout_v[...].astype(F32)
    dyflat_v[0:tok, :] = (gate_v[0] * dout_f).astype(BF16)
    dyflat_v[tok:2 * tok, :] = (gate_v[1] * dout_f).astype(BF16)
    for d in (2, 4, 3, 5, 6, 7, 1, 0):
        pick0 = jnp.where(rank_v[d:d + 1, :] == slot, 1.0, 0.0).astype(BF16)
        pick1 = jnp.where(rank_v[16 + d:17 + d, :] == slot, 1.0, 0.0).astype(BF16)
        block = (dot_nn(pick0, dyflat_v[0:tok]) + dot_nn(pick1, dyflat_v[tok:2 * tok])).astype(BF16)
        if d == 0:
            rdy[0:ROWS] = block
        else:
            sdy[d * ROWS:(d + 1) * ROWS] = block
            remote(1, sdy, rdy, d).start()

    hid = 512
    loads[4].wait()
    loads[5].wait()
    def fwd_chunk(c, carry):
        @pl.when(c > 0)
        def _():
            remote(0, sx, rx, 2 * c).wait_recv()

        remote(0, sx, rx, 2 * c + 1).wait_recv()
        rows = pl.ds(pl.multiple_of(c * (2 * ROWS), 2 * ROWS), 2 * ROWS)
        x_c = rx[rows]

        def fwd_tile(j, inner):
            cols = pl.ds(pl.multiple_of(j * hid, hid), hid)
            a = dot_nn(x_c, win_v[:, cols])
            sq = a * a
            t = jnp.tanh(SQRT_2_PI * (a + CUBIC * (a * sq)))
            cdf = 0.5 * (1.0 + t)
            h_v[rows, cols] = (a * cdf).astype(BF16)
            gp_v[rows, cols] = cdf + (0.5 * a) * (1.0 - t * t) * (SQRT_2_PI * (1.0 + (3.0 * CUBIC) * sq))
            return inner

        lax.fori_loop(0, d_hid // hid, fwd_tile, 0)
        sy[rows] = dot_nn(h_v[rows], wout_v[...]).astype(BF16)

        @pl.when(c > 0)
        def _():
            remote(2, sy, ry, 2 * c).start()

        remote(2, sy, ry, 2 * c + 1).start()
        return carry

    lax.fori_loop(0, N_DEV // 2, fwd_chunk, 0)
    ry[0:ROWS] = sy[0:ROWS]

    slot_l = lax.broadcasted_iota(jnp.int32, (tok, ROWS), 1).astype(F32)
    for d in range(N_DEV):
        span = slice(d * ROWS, (d + 1) * ROWS)
        own0 = jnp.where(cols_v[:, d:d + 1] == slot_l, 1.0, 0.0)
        own1 = jnp.where(cols_v[:, 16 + d:17 + d] == slot_l, 1.0, 0.0)
        q0_v[:, span] = own0.astype(BF16)
        q1_v[:, span] = own1.astype(BF16)
        q01_ref[:, span] = (own0 + own1).astype(BF16)

    def bwd_chunk(c, carry):
        @pl.when(c > 0)
        def _():
            remote(1, sdy, rdy, 2 * c).wait_recv()

        remote(1, sdy, rdy, 2 * c + 1).wait_recv()
        rows = pl.ds(pl.multiple_of(c * (2 * ROWS), 2 * ROWS), 2 * ROWS)
        dy_c = rdy[rows]

        def bwd_tile(j, inner):
            cols = pl.ds(pl.multiple_of(j * hid, hid), hid)
            dh = dot_nt(dy_c, wout_v[cols, :])
            da_v[rows, cols] = (dh * gp_v[rows, cols]).astype(BF16)
            return inner

        lax.fori_loop(0, d_hid // hid, bwd_tile, 0)
        sdx[rows] = dot_nt(da_v[rows], win_v[...]).astype(BF16)
        return carry

    lax.fori_loop(0, N_DEV // 2, bwd_chunk, 0)
    rdx[0:ROWS] = sdx[0:ROWS]
    for d in DX_EARLY:
        remote(3, sdx, rdx, d).start()

    xt_v[...] = rx[...].T
    wt = 256

    def grad_tile(j, carry):
        cols = pl.ds(pl.multiple_of(j * wt, wt), wt)
        gwout_ref[cols, :] = dot_tn(h_v[:, cols], rdy[...])
        gwin_ref[:, cols] = dot_nn(xt_v[...], da_v[:, cols])
        return carry

    lax.fori_loop(0, d_hid // wt, grad_tile, 0)

    for d in range(1, 6):
        remote(2, sy, ry, d).wait_recv()
    span = slice(0, 6 * ROWS)
    y0 = dot_nn(q0_v[:, span], ry[span])
    y1 = dot_nn(q1_v[:, span], ry[span])
    for d in (6, 7):
        remote(2, sy, ry, d).wait_recv()
    span = slice(6 * ROWS, 8 * ROWS)
    y0 = y0 + dot_nn(q0_v[:, span], ry[span])
    y1 = y1 + dot_nn(q1_v[:, span], ry[span])
    g0 = gate_v[0]
    g1 = gate_v[1]
    dout_f = dout_v[...].astype(F32)
    dg0 = jnp.sum(dout_f * y0, axis=1, keepdims=True)
    dg1 = jnp.sum(dout_f * y1, axis=1, keepdims=True)
    mean = g0 * dg0 + g1 * dg1
    d_log = (jnp.where(lane8 == cols_v[:, 32:33], g0 * (dg0 - mean), 0.0)
             + jnp.where(lane8 == cols_v[:, 48:49], g1 * (dg1 - mean), 0.0)).astype(BF16)
    for i in range(2):
        wg_part[i] = dot_tn(d_log, x_v[:, i * half:(i + 1) * half])

    def wg_copy(i, src, dst, d):
        return pltpu.make_async_remote_copy(
            src_ref=src, dst_ref=dst, send_sem=wg_send.at[i], recv_sem=wg_recv.at[i],
            device_id=(peer(d),), device_id_type=MESH)

    chip = 2 * row + col
    to_mate = wg_copy(0, wg_part.at[1 - core], wg_mate, 1)
    to_mate.start()
    out_ref[...] = (g0 * y0 + g1 * y1).astype(BF16)
    acc_ref[...] = dot_nn(d_log, wgt_ref[...])
    to_mate.wait_recv()
    wg_chip[chip] = wg_part[core] + wg_mate[...]
    to_chips = [wg_copy(1 + i, wg_chip.at[chip], wg_chip.at[chip], 2 * (i + 1)) for i in range(3)]
    for cp in to_chips:
        cp.start()
    for d in DX_LATE:
        remote(3, sdx, rdx, d).start()

    for cp in to_chips:
        cp.wait_recv()
    gwg_ref[core] = (wg_chip[0] + wg_chip[1]) + (wg_chip[2] + wg_chip[3])
    swap = wg_copy(4, gwg_ref.at[core], gwg_ref.at[core], 1)
    swap.start()
    to_mate.wait_send()
    for d in range(1, N_DEV):
        remote(0, sx, rx, d).wait_send()
        remote(1, sdy, rdy, d).wait_send()
        remote(2, sy, ry, d).wait_send()
    for cp in to_chips:
        cp.wait_send()
    swap.wait()
    for d in range(1, N_DEV):
        remote(3, sdx, rdx, d).wait()


def finish_kernel(out_v, gwin_v, gwout_v, gwg_v, acc_v, q01_v, dx_v,
                  out_hbm, gx_hbm, gwin_hbm, gwout_hbm, gwg_hbm, gx_v, sem):
    half = gwg_v.shape[2]
    pieces = [(gwin_v, gwin_hbm), (gwout_v, gwout_hbm), (out_v, out_hbm), (gwg_v.at[0], gwg_hbm.at[:, pl.ds(0, half)]),
              (gwg_v.at[1], gwg_hbm.at[:, pl.ds(half, half)]), (gx_v, gx_hbm)]
    stores = [pltpu.make_async_copy(src, dst, sem.at[i]) for i, (src, dst) in enumerate(pieces)]
    for st in stores[:-1]:
        st.start()
    gx_v[...] = (acc_v[...] + dot_nn(q01_v[...], dx_v[...])).astype(BF16)
    stores[-1].start()
    for st in stores:
        st.wait()


def local_block(tokens, grad_out, expert_ids, w_gate, w_in, w_out):
    tok, d_model = tokens.shape
    n_exp = w_gate.shape[1]
    d_hid = w_in.shape[2]
    slots = n_exp * ROWS
    vmem = pl.BlockSpec(memory_space=pltpu.VMEM)
    hbm = pl.BlockSpec(memory_space=pl.ANY)
    blocks = pltpu.VMEM((slots, d_model), BF16)
    args = [pltpu.with_memory_space_constraint(a, pltpu.HBM)
            for a in (expert_ids.T, w_gate.T, tokens, grad_out, w_in[0], w_out[0])]
    kept = pl.pallas_call(
        moe_kernel,
        out_shape=(pltpu.VMEM((tok, d_model), BF16), pltpu.VMEM((d_model, d_hid), F32), pltpu.VMEM((d_hid, d_model), F32),
                   pltpu.VMEM((2, n_exp, d_model // 2), F32), pltpu.VMEM((tok, d_model), F32),
                   pltpu.VMEM((tok, slots), BF16), pltpu.VMEM((slots, d_model), BF16)),
        in_specs=[hbm] * 6,
        out_specs=(vmem,) * 7,
        scratch_shapes=[
            pltpu.VMEM((2, tok), jnp.int32), pltpu.VMEM((n_exp, d_model), BF16),
            pltpu.VMEM((tok, d_model), BF16), pltpu.VMEM((tok, d_model), BF16),
            pltpu.VMEM((d_model, d_hid), BF16), pltpu.VMEM((d_hid, d_model), BF16),
            pltpu.VMEM((48, tok), F32),
            pltpu.VMEM((tok, slots), BF16), pltpu.VMEM((tok, slots), BF16),
            pltpu.VMEM((2 * tok, d_model), BF16), pltpu.VMEM((2, tok, 1), F32), pltpu.VMEM((tok, 128), F32),
            blocks, blocks, blocks, blocks, blocks, blocks, blocks,
            pltpu.VMEM((slots, d_hid), BF16), pltpu.VMEM((slots, d_hid), F32), pltpu.VMEM((slots, d_hid), BF16),
            pltpu.VMEM((d_model, slots), BF16), pltpu.VMEM((ROWS, 2 * ROWS), BF16),
            pltpu.VMEM((2, n_exp, d_model // 2), F32), pltpu.VMEM((n_exp, d_model // 2), F32), pltpu.VMEM((4, n_exp, d_model // 2), F32),
            pltpu.SemaphoreType.DMA((6,)), pltpu.SemaphoreType.DMA((4, n_exp)), pltpu.SemaphoreType.DMA((4, n_exp)),
            pltpu.SemaphoreType.DMA((5,)), pltpu.SemaphoreType.DMA((5,)),
        ],
        compiler_params=pltpu.CompilerParams(collective_id=0, has_side_effects=True, vmem_limit_bytes=46 * 1024 * 1024),
        name='moe_step',
    )(*args)
    out, gx, gwin, gwout, gwg = pl.pallas_call(
        finish_kernel,
        out_shape=(jax.ShapeDtypeStruct((tok, d_model), BF16), jax.ShapeDtypeStruct((tok, d_model), BF16),
                   jax.ShapeDtypeStruct((d_model, d_hid), F32), jax.ShapeDtypeStruct((d_hid, d_model), F32),
                   jax.ShapeDtypeStruct((n_exp, d_model), F32)),
        in_specs=[vmem] * 7,
        out_specs=(hbm,) * 5,
        scratch_shapes=[pltpu.VMEM((tok, d_model), BF16), pltpu.SemaphoreType.DMA((6,))],
        compiler_params=pltpu.CompilerParams(vmem_limit_bytes=16 * 1024 * 1024),
        name='moe_finish',
    )(*kept)
    return out, gx, gwin[None], gwout[None], gwg.T


def solution(mesh):
    return jax.shard_map(local_block, mesh=mesh, in_specs=(P('ep'), P('ep'), P('ep'), P(), P('ep'), P('ep')), out_specs=(P('ep'), P('ep'), P('ep'), P('ep'), P()), check_vma=False)
```

```python
import functools

import jax
import jax.numpy as jnp
from jax import lax
from jax.experimental import pallas as pl
from jax.experimental.pallas import tpu as pltpu
from jax.sharding import PartitionSpec as P

N_DEV = 8
DX_EARLY = (1, 2, 4, 6, 3)
DX_LATE = (7, 5)
ROWS = 128
MESH = pl.DeviceIdType.MESH
F32 = jnp.float32
BF16 = jnp.bfloat16
SQRT_2_PI = 0.7978845608028654
CUBIC = 0.044715


def dot_nn(a, b):
    return lax.dot_general(a, b, (((1,), (0,)), ((), ())), preferred_element_type=F32)


def dot_nt(a, b):
    return lax.dot_general(a, b, (((1,), (1,)), ((), ())), preferred_element_type=F32)


def dot_tn(a, b):
    return lax.dot_general(a, b, (((0,), (0,)), ((), ())), preferred_element_type=F32)


def moe_kernel(ids_hbm, wgt_hbm, x_hbm, dout_hbm, win_hbm, wout_hbm,
               out_ref, gwin_ref, gwout_ref, gwg_ref, acc_ref, q01_ref, rdx,
               ids_ref, wgt_ref, x_v, dout_v, win_v, wout_v, rank_v, q0_v, q1_v, dyflat_v, gate_v, cols_v,
               sx, rx, sdy, rdy, sy, ry, sdx, h_v, gp_v, da_v, xt_v, before_v, wg_part, wg_mate, wg_chip,
               load_sem, send_sem, recv_sem, wg_send, wg_recv):
    tok = x_v.shape[0]
    d_hid = win_v.shape[1]
    half = x_v.shape[1] // 2
    me = lax.axis_index('ep')
    core, col, row = me % 2, (me // 2) % 2, me // 4

    def peer(d):
        return 4 * ((row + d // 4) % 2) + 2 * ((col + (d // 2) % 2) % 2) + (core + d % 2) % 2

    def remote(phase, src, dst, d):
        return pltpu.make_async_remote_copy(
            src_ref=src.at[pl.ds(d * ROWS, ROWS)], dst_ref=dst.at[pl.ds(d * ROWS, ROWS)], send_sem=send_sem.at[phase, d], recv_sem=recv_sem.at[phase, d],
            device_id=(peer(d),), device_id_type=MESH)

    loads = [pltpu.make_async_copy(src, dst, load_sem.at[i]) for i, (src, dst) in enumerate(
        ((ids_hbm, ids_ref), (x_hbm, x_v), (wgt_hbm, wgt_ref), (dout_hbm, dout_v), (win_hbm, win_v), (wout_hbm, wout_v)))]
    for ld in loads[:2]:
        ld.start()
    barrier = pltpu.get_barrier_semaphore()
    for d in range(1, N_DEV):
        pl.semaphore_signal(barrier, inc=1, device_id=(peer(d),), device_id_type=MESH)
    for ld in loads[2:]:
        ld.start()

    rel = lax.broadcasted_iota(jnp.int32, (16, tok), 0) ^ me
    lane2 = lax.broadcasted_iota(jnp.int32, (ROWS, 2 * ROWS), 1)
    before_v[...] = jnp.where((lax.broadcasted_iota(jnp.int32, (ROWS, 2 * ROWS), 0) < lane2) | (lane2 >= ROWS), 1.0, 0.0).astype(BF16)
    slot = lax.broadcasted_iota(jnp.int32, (ROWS, tok), 0).astype(F32)
    loads[0].wait()
    ids0 = ids_ref[0:1, :]
    ids1 = ids_ref[1:2, :]
    hit0 = rel == ids0
    hit1 = rel == ids1
    hot = jnp.where(hit0 | hit1, 1.0, 0.0).astype(BF16)
    groups = [slice(g * ROWS, (g + 1) * ROWS) for g in range(tok // ROWS)]
    counts = dot_nn(jnp.concatenate([hot[:, g] for g in groups], axis=0), before_v[...])
    rank, base = [], 0.0
    for g in range(tok // ROWS):
        part = counts[16 * g:16 * (g + 1)]
        rank.append(part[:, 0:ROWS] + base)
        base = base + part[:, ROWS:2 * ROWS]
    rank = jnp.concatenate(rank, axis=1)
    rank0 = jnp.where(hit0, rank, -1.0)
    rank1 = jnp.where(hit1, rank, -1.0)
    rank_v[32:48, :] = jnp.where(hit0 | hit1, rank, -1.0)
    rank_v[0:16, :] = rank0
    rank_v[16:32, :] = rank1

    loads[1].wait()
    for group in ((2,), (4, 6), (3, 5), (7, 1), (0,)):
        pick = jnp.concatenate([jnp.where(rank_v[32 + d:33 + d, :] == slot, 1.0, 0.0).astype(BF16) for d in group], axis=0)
        blocks = dot_nn(pick, x_v[...]).astype(BF16)
        for i, d in enumerate(group):
            block = blocks[i * ROWS:(i + 1) * ROWS]
            if d == 0:
                rx[0:ROWS] = block
            else:
                sx[d * ROWS:(d + 1) * ROWS] = block
                if d == 2:
                    pl.semaphore_wait(barrier, N_DEV - 1)
                remote(0, sx, rx, d).start()

    stack = jnp.concatenate([rank0, rank1, jnp.broadcast_to(ids0.astype(F32), (16, tok)),
                             jnp.broadcast_to(ids1.astype(F32), (16, tok)), jnp.zeros((64, tok), F32)], axis=0)
    cols_v[...] = stack.T
    loads[2].wait()
    logits = dot_nt(x_v[...], wgt_ref[...])
    lane8 = lax.broadcasted_iota(jnp.int32, (tok, N_DEV), 1).astype(F32)
    sel0 = jnp.sum(jnp.where(lane8 == cols_v[:, 32:33], logits, 0.0), axis=1, keepdims=True)
    sel1 = jnp.sum(jnp.where(lane8 == cols_v[:, 48:49], logits, 0.0), axis=1, keepdims=True)
    top = jnp.maximum(sel0, sel1)
    e0 = jnp.exp(sel0 - top)
    e1 = jnp.exp(sel1 - top)
    gate_v[0] = e0 / (e0 + e1)
    gate_v[1] = e1 / (e0 + e1)
    loads[3].wait()
    dout_f = dout_v[...].astype(F32)
    dyflat_v[0:tok, :] = (gate_v[0] * dout_f).astype(BF16)
    dyflat_v[tok:2 * tok, :] = (gate_v[1] * dout_f).astype(BF16)
    for d in (2, 4, 3, 5, 6, 7, 1, 0):
        pick0 = jnp.where(rank_v[d:d + 1, :] == slot, 1.0, 0.0).astype(BF16)
        pick1 = jnp.where(rank_v[16 + d:17 + d, :] == slot, 1.0, 0.0).astype(BF16)
        block = (dot_nn(pick0, dyflat_v[0:tok]) + dot_nn(pick1, dyflat_v[tok:2 * tok])).astype(BF16)
        if d == 0:
            rdy[0:ROWS] = block
        else:
            sdy[d * ROWS:(d + 1) * ROWS] = block
            remote(1, sdy, rdy, d).start()

    hid = 512
    loads[4].wait()
    loads[5].wait()
    def fwd_chunk(c, carry):
        @pl.when(c > 0)
        def _():
            remote(0, sx, rx, 2 * c).wait_recv()

        remote(0, sx, rx, 2 * c + 1).wait_recv()
        rows = pl.ds(pl.multiple_of(c * (2 * ROWS), 2 * ROWS), 2 * ROWS)
        x_c = rx[rows]

        def fwd_tile(j, inner):
            cols = pl.ds(pl.multiple_of(j * hid, hid), hid)
            a = dot_nn(x_c, win_v[:, cols])
            sq = a * a
            t = jnp.tanh(SQRT_2_PI * (a + CUBIC * (a * sq)))
            cdf = 0.5 * (1.0 + t)
            h_v[rows, cols] = (a * cdf).astype(BF16)
            gp_v[rows, cols] = cdf + (0.5 * a) * (1.0 - t * t) * (SQRT_2_PI * (1.0 + (3.0 * CUBIC) * sq))
            return inner

        lax.fori_loop(0, d_hid // hid, fwd_tile, 0)
        sy[rows] = dot_nn(h_v[rows], wout_v[...]).astype(BF16)

        @pl.when(c > 0)
        def _():
            remote(2, sy, ry, 2 * c).start()

        remote(2, sy, ry, 2 * c + 1).start()
        return carry

    lax.fori_loop(0, N_DEV // 2, fwd_chunk, 0)
    ry[0:ROWS] = sy[0:ROWS]

    slot_l = lax.broadcasted_iota(jnp.int32, (tok, ROWS), 1).astype(F32)
    for d in range(N_DEV):
        span = slice(d * ROWS, (d + 1) * ROWS)
        own0 = jnp.where(cols_v[:, d:d + 1] == slot_l, 1.0, 0.0)
        own1 = jnp.where(cols_v[:, 16 + d:17 + d] == slot_l, 1.0, 0.0)
        q0_v[:, span] = own0.astype(BF16)
        q1_v[:, span] = own1.astype(BF16)
        q01_ref[:, span] = (own0 + own1).astype(BF16)

    def bwd_chunk(c, carry):
        @pl.when(c > 0)
        def _():
            remote(1, sdy, rdy, 2 * c).wait_recv()

        remote(1, sdy, rdy, 2 * c + 1).wait_recv()
        rows = pl.ds(pl.multiple_of(c * (2 * ROWS), 2 * ROWS), 2 * ROWS)
        dy_c = rdy[rows]

        def bwd_tile(j, inner):
            cols = pl.ds(pl.multiple_of(j * hid, hid), hid)
            dh = dot_nt(dy_c, wout_v[cols, :])
            da_v[rows, cols] = (dh * gp_v[rows, cols]).astype(BF16)
            return inner

        lax.fori_loop(0, d_hid // hid, bwd_tile, 0)
        sdx[rows] = dot_nt(da_v[rows], win_v[...]).astype(BF16)
        return carry

    lax.fori_loop(0, N_DEV // 2, bwd_chunk, 0)
    rdx[0:ROWS] = sdx[0:ROWS]
    for d in DX_EARLY:
        remote(3, sdx, rdx, d).start()

    xt_v[...] = rx[...].T
    wt = 256

    def grad_tile(j, carry):
        cols = pl.ds(pl.multiple_of(j * wt, wt), wt)
        gwout_ref[cols, :] = dot_tn(h_v[:, cols], rdy[...])
        gwin_ref[:, cols] = dot_nn(xt_v[...], da_v[:, cols])
        return carry

    lax.fori_loop(0, d_hid // wt, grad_tile, 0)

    for d in range(1, 6):
        remote(2, sy, ry, d).wait_recv()
    span = slice(0, 6 * ROWS)
    y0 = dot_nn(q0_v[:, span], ry[span])
    y1 = dot_nn(q1_v[:, span], ry[span])
    for d in (6, 7):
        remote(2, sy, ry, d).wait_recv()
    span = slice(6 * ROWS, 8 * ROWS)
    y0 = y0 + dot_nn(q0_v[:, span], ry[span])
    y1 = y1 + dot_nn(q1_v[:, span], ry[span])
    g0 = gate_v[0]
    g1 = gate_v[1]
    dout_f = dout_v[...].astype(F32)
    dg0 = jnp.sum(dout_f * y0, axis=1, keepdims=True)
    dg1 = jnp.sum(dout_f * y1, axis=1, keepdims=True)
    mean = g0 * dg0 + g1 * dg1
    d_log = (jnp.where(lane8 == cols_v[:, 32:33], g0 * (dg0 - mean), 0.0)
             + jnp.where(lane8 == cols_v[:, 48:49], g1 * (dg1 - mean), 0.0)).astype(BF16)
    for i in range(2):
        wg_part[i] = dot_tn(d_log, x_v[:, i * half:(i + 1) * half])

    def wg_copy(i, src, dst, d):
        return pltpu.make_async_remote_copy(
            src_ref=src, dst_ref=dst, send_sem=wg_send.at[i], recv_sem=wg_recv.at[i],
            device_id=(peer(d),), device_id_type=MESH)

    chip = 2 * row + col
    to_mate = wg_copy(0, wg_part.at[1 - core], wg_mate, 1)
    to_mate.start()
    out_ref[...] = (g0 * y0 + g1 * y1).astype(BF16)
    acc_ref[...] = dot_nn(d_log, wgt_ref[...])
    to_mate.wait_recv()
    wg_chip[chip] = wg_part[core] + wg_mate[...]
    to_chips = [wg_copy(1 + i, wg_chip.at[chip], wg_chip.at[chip], 2 * (i + 1)) for i in range(3)]
    for cp in to_chips:
        cp.start()
    for d in DX_LATE:
        remote(3, sdx, rdx, d).start()

    for cp in to_chips:
        cp.wait_recv()
    gwg_ref[core] = (wg_chip[0] + wg_chip[1]) + (wg_chip[2] + wg_chip[3])
    swap = wg_copy(4, gwg_ref.at[core], gwg_ref.at[core], 1)
    swap.start()
    to_mate.wait_send()
    for d in range(1, N_DEV):
        remote(0, sx, rx, d).wait_send()
        remote(1, sdy, rdy, d).wait_send()
        remote(2, sy, ry, d).wait_send()
    for cp in to_chips:
        cp.wait_send()
    swap.wait()
    for d in range(1, N_DEV):
        remote(3, sdx, rdx, d).wait()


def finish_kernel(out_v, gwin_v, gwout_v, gwg_v, acc_v, q01_v, dx_v,
                  out_hbm, gx_hbm, gwin_hbm, gwout_hbm, gwg_hbm, gx_v, sem):
    half = gwg_v.shape[2]
    pieces = [(gwin_v, gwin_hbm), (gwout_v, gwout_hbm), (out_v, out_hbm), (gwg_v.at[0], gwg_hbm.at[:, pl.ds(0, half)]),
              (gwg_v.at[1], gwg_hbm.at[:, pl.ds(half, half)]), (gx_v, gx_hbm)]
    stores = [pltpu.make_async_copy(src, dst, sem.at[i]) for i, (src, dst) in enumerate(pieces)]
    for st in stores[:-1]:
        st.start()
    gx_v[...] = (acc_v[...] + dot_nn(q01_v[...], dx_v[...])).astype(BF16)
    stores[-1].start()
    for st in stores:
        st.wait()


def local_block(tokens, grad_out, expert_ids, w_gate, w_in, w_out):
    tok, d_model = tokens.shape
    n_exp = w_gate.shape[1]
    d_hid = w_in.shape[2]
    slots = n_exp * ROWS
    vmem = pl.BlockSpec(memory_space=pltpu.VMEM)
    hbm = pl.BlockSpec(memory_space=pl.ANY)
    blocks = pltpu.VMEM((slots, d_model), BF16)
    args = [pltpu.with_memory_space_constraint(a, pltpu.HBM)
            for a in (expert_ids.T, w_gate.T, tokens, grad_out, w_in[0], w_out[0])]
    kept = pl.pallas_call(
        moe_kernel,
        out_shape=(pltpu.VMEM((tok, d_model), BF16), pltpu.VMEM((d_model, d_hid), F32), pltpu.VMEM((d_hid, d_model), F32),
                   pltpu.VMEM((2, n_exp, d_model // 2), F32), pltpu.VMEM((tok, d_model), F32),
                   pltpu.VMEM((tok, slots), BF16), pltpu.VMEM((slots, d_model), BF16)),
        in_specs=[hbm] * 6,
        out_specs=(vmem,) * 7,
        scratch_shapes=[
            pltpu.VMEM((2, tok), jnp.int32), pltpu.VMEM((n_exp, d_model), BF16),
            pltpu.VMEM((tok, d_model), BF16), pltpu.VMEM((tok, d_model), BF16),
            pltpu.VMEM((d_model, d_hid), BF16), pltpu.VMEM((d_hid, d_model), BF16),
            pltpu.VMEM((48, tok), F32),
            pltpu.VMEM((tok, slots), BF16), pltpu.VMEM((tok, slots), BF16),
            pltpu.VMEM((2 * tok, d_model), BF16), pltpu.VMEM((2, tok, 1), F32), pltpu.VMEM((tok, 128), F32),
            blocks, blocks, blocks, blocks, blocks, blocks, blocks,
            pltpu.VMEM((slots, d_hid), BF16), pltpu.VMEM((slots, d_hid), F32), pltpu.VMEM((slots, d_hid), BF16),
            pltpu.VMEM((d_model, slots), BF16), pltpu.VMEM((ROWS, 2 * ROWS), BF16),
            pltpu.VMEM((2, n_exp, d_model // 2), F32), pltpu.VMEM((n_exp, d_model // 2), F32), pltpu.VMEM((4, n_exp, d_model // 2), F32),
            pltpu.SemaphoreType.DMA((6,)), pltpu.SemaphoreType.DMA((4, n_exp)), pltpu.SemaphoreType.DMA((4, n_exp)),
            pltpu.SemaphoreType.DMA((5,)), pltpu.SemaphoreType.DMA((5,)),
        ],
        compiler_params=pltpu.CompilerParams(collective_id=0, has_side_effects=True, vmem_limit_bytes=46 * 1024 * 1024),
        name='moe_step',
    )(*args)
    out, gx, gwin, gwout, gwg = pl.pallas_call(
        finish_kernel,
        out_shape=(jax.ShapeDtypeStruct((tok, d_model), BF16), jax.ShapeDtypeStruct((tok, d_model), BF16),
                   jax.ShapeDtypeStruct((d_model, d_hid), F32), jax.ShapeDtypeStruct((d_hid, d_model), F32),
                   jax.ShapeDtypeStruct((n_exp, d_model), F32)),
        in_specs=[vmem] * 7,
        out_specs=(hbm,) * 5,
        scratch_shapes=[pltpu.VMEM((tok, d_model), BF16), pltpu.SemaphoreType.DMA((6,))],
        compiler_params=pltpu.CompilerParams(vmem_limit_bytes=16 * 1024 * 1024),
        name='moe_finish',
    )(*kept)
    return out, gx, gwin[None], gwout[None], gwg.T


def solution(mesh):
    return jax.shard_map(local_block, mesh=mesh, in_specs=(P('ep'), P('ep'), P('ep'), P(), P('ep'), P('ep')), out_specs=(P('ep'), P('ep'), P('ep'), P('ep'), P()), check_vma=False)
```
